32 devices in a mesh: gx: 8 (over y, x, core), gy: 4 (over z).
Axes of the slice: x: 2, y: 2, z: 4, core: 2. Of those that a mesh axis runs over, the one named last changes fastest.
Arguments:
- core_one: bfloat16 [200, 128], replicated, may hold values from -6 to 6
- core_two: bfloat16 [200, 4096], replicated, may hold values from -1 to 1
- core_three: bfloat16 [250, 256], replicated, may hold values from -1 to 1
- dense_rows: bfloat16 [2048, 128], P(('gx', 'gy')), may hold values from -6 to 6
- w_top: bfloat16 [256, 256], replicated, may hold values from -0.375 to 0.375
- bias_top: float32 [256], replicated, may hold values from -3 to 3
- w_out: float32 [256], replicated, may hold values from -0.75 to 0.75
- labels: int32 [2048], P(('gx', 'gy')), may hold values 0 or 1
- bag_ids: int32 [32, 256], P(('gx', 'gy')), may hold values from 0 to 63, never falling along the last dimension, each value on 1 to 8 neighbouring positions
- digit_one: int32 [32, 256], P(('gx', 'gy')), may hold values from 0 to 199
- digit_two: int32 [32, 256], P(('gx', 'gy')), may hold values from 0 to 199
- digit_three: int32 [32, 256], P(('gx', 'gy')), may hold values from 0 to 249
Outputs:
- core_grad: float32 [908800], P(('gx', 'gy'))
- top_grad: float32 [258, 256], replicated
The draws below stay inside these ranges and needn't reach their ends.
Inputs may be any that keep to these rules, and one draw needn't show every extreme that they name: `bag_ids`: along a row, never falling; every sample of the block gets 1 to 8 lookups, one exactly 8.
All inputs are finite; a program needn't handle non-finite values. No bound on the sum of `labels` on one device may be relied on, other than what follows from the above.
Results may differ from the reference program's by a relative error of at most 0.0018.
The reference program's roundings to bfloat16 on the way (of `joined` and `dpre`) count: a program that leaves them out, or rounds other values in their place, can miss the bound.
Values sent between devices are 32-bit elements; how exact they have to be, the bound alone decides.
A program may use at most 64 MiB of HBM per device.

```python
import math
import jax
import jax.numpy as jnp
import numpy as np
from jax import lax

N1 = 200
N2 = 200
N3 = 250
D1 = 4
D2 = 4
D3 = 8
R = 32
HID = 256
BAG_MOST = 8
BATCH_DEV = 64
DIM = 128
LOOKS = 256
BATCH = 2048
N_GX = 8
N_GY = 4
DEVICES = 32


def touch_ends(drawn, rng, low, largest):
    longest = drawn.shape.index(max(drawn.shape))
    spots = []
    for shift in (0, 1):
        where = [jax.random.randint(jax.random.fold_in(rng, axis), (), 0, length) for axis, length in enumerate(drawn.shape)]
        where[longest] = (where[longest] + shift) % drawn.shape[longest]
        spots.append(tuple(where))
    return drawn.at[spots[0]].set(low).at[spots[1]].set(largest)


def spiked(array, stream_key, source, target, blocks, factor):
    owner, partner = [(jnp.arange(array.shape[position]) // (array.shape[position] // blocks)).reshape([-1 if axis == position else 1 for axis in range(array.ndim)]) for position in (source, target)]
    chosen = jax.random.permutation(stream_key, blocks)[partner]
    strong = (owner == chosen) | (owner == (partner + blocks // 2) % blocks)
    return jnp.where(strong, factor * array, array)


def levels(stream_key, dims, cuts, smallest, top_value):
    def one(dim, shards_of):
        steps = jax.random.uniform(jax.random.fold_in(jax.random.fold_in(stream_key, 6), dim), (shards_of,), jnp.float32, smallest / len(cuts), top_value / len(cuts))
        return jnp.repeat(jnp.exp(steps), dims[dim] // shards_of).reshape((-1,) + (1,) * (len(dims) - dim - 1))

    factor_of = one(*cuts[0])
    for cut in cuts[1:]:
        factor_of = factor_of * one(*cut)
    return factor_of


def split_up(amount, total, reach, slope):
    loads = [(1 << 20) // math.isqrt(standing ** slope) + 1 for standing in range(2, amount + 1)]
    spare, given = total - reach - (amount - 1), [1] * (amount - 1)
    while spare > 0:
        movable = [i for i in range(amount - 1) if given[i] < reach]
        pool, left = sum([loads[i] for i in movable]), spare
        for i in movable:
            more = min(reach - given[i], max(1, left * loads[i] // pool), spare)
            given[i] = given[i] + more
            spare = spare - more
    return np.array([reach] + given)


def uneven_parts(key, number_of, total, reach, slope):
    if number_of == 2:
        one = jax.random.randint(key, (), max(1, total - reach), min(reach, total - 1) + 1)
        return jnp.stack([one, total - one])
    sizes = jnp.asarray(split_up(number_of, total, reach, slope), jnp.int32)
    pairs = (number_of - 1) // 2
    giver, receiver = sizes[1:1 + 2 * pairs:2], sizes[2:2 + 2 * pairs:2]
    room = jnp.minimum(giver - 1, reach - receiver)
    passed = jax.random.randint(jax.random.fold_in(key, 1), (pairs,), 0, 1 << 20) % (room + 1)
    sizes = sizes.at[1:1 + 2 * pairs:2].set(giver - passed).at[2:2 + 2 * pairs:2].set(receiver + passed)
    return sizes[jax.random.permutation(jax.random.fold_in(key, 2), number_of)]


def bell_draw(stream_key, shape, spread, most, cuts=(), kind=jnp.bfloat16):
    level = levels(stream_key, shape, cuts, -0.22, 0.18) if cuts else 1.0
    array = jax.random.normal(stream_key, shape, jnp.float32) * spread * level
    return jnp.minimum(jnp.maximum(array, -most), most).astype(kind)


def heavy_noise(key, shape, width, limit, cuts, heavy, held_as=jnp.bfloat16):
    result = width * jax.random.normal(key, shape, jnp.float32)
    if cuts:
        result = result * levels(key, shape, cuts, -0.22, 0.18)
    return jnp.clip(spiked(result, jax.random.fold_in(key, 3), *heavy), -limit, limit).astype(held_as)


def setup_inputs(seed: int = 0) -> dict:
    keys = jax.random.split(jax.random.key(seed), 13)
    core_one = bell_draw(keys[0], (N1, D1 * R), 1.0, 6.0)
    core_two = bell_draw(keys[1], (N2, R * D2 * R), R ** -0.5, 1.0)
    core_three = bell_draw(keys[2], (N3, R * D3), R ** -0.5, 1.0)
    dense_rows = heavy_noise(keys[3], (BATCH, DIM), 1.0, 6.0, ((0, 32),), (0, 1, 32, 2.75))
    w_top = bell_draw(keys[4], (2 * DIM, HID), (2 * DIM) ** -0.5, 0.375)
    bias_top = bell_draw(keys[5], (HID,), 0.5, 3.0, (), jnp.float32)
    w_out = bell_draw(keys[6], (HID,), (HID // 4) ** -0.5, 0.75, (), jnp.float32)
    labels = touch_ends((jax.random.randint(keys[7], (BATCH,), 0, 4) < 1).astype(jnp.int32), jax.random.fold_in(keys[7], 1), 0, 1)
    bag_ids = jax.vmap(lambda own: jnp.searchsorted(jnp.cumsum(uneven_parts(own, BATCH_DEV, LOOKS, BAG_MOST, 1)), jnp.arange(LOOKS), side="right"))(jax.random.split(keys[8], DEVICES)).reshape((DEVICES, LOOKS)).astype(jnp.int32)
    digit_one = touch_ends(jax.random.randint(keys[9], (DEVICES, LOOKS), 0, N1), jax.random.fold_in(keys[9], 1), 0, N1 - 1).astype(jnp.int32)
    digit_two = touch_ends(jax.random.randint(keys[10], (DEVICES, LOOKS), 0, N2), jax.random.fold_in(keys[10], 1), 0, N2 - 1).astype(jnp.int32)
    digit_three = touch_ends(jax.random.randint(keys[11], (DEVICES, LOOKS), 0, N3), jax.random.fold_in(keys[11], 1), 0, N3 - 1).astype(jnp.int32)
    return {"core_one": core_one, "core_two": core_two, "core_three": core_three, "dense_rows": dense_rows, "w_top": w_top, "bias_top": bias_top, "w_out": w_out, "labels": labels, "bag_ids": bag_ids, "digit_one": digit_one, "digit_two": digit_two, "digit_three": digit_three}


def reference(core_one, core_two, core_three, dense_rows, w_top, bias_top, w_out, labels, bag_ids, digit_one, digit_two, digit_three):
    high = lax.Precision.HIGHEST
    groups = N_GX * N_GY
    dense_view = dense_rows.reshape(groups, BATCH_DEV, DIM)
    label_view = labels.reshape(groups, BATCH_DEV)

    def device_terms(carry, item):
        dense_block, label_block, bags, first_digit, second_digit, third_digit = item
        first = core_one[first_digit].astype(jnp.float32).reshape(-1, D1, R)
        middle = core_two[second_digit].astype(jnp.float32).reshape(-1, R, D2 * R)
        last = core_three[third_digit].astype(jnp.float32).reshape(-1, R, D3)
        left = jnp.einsum("nia,nab->nib", first, middle, precision=high).reshape(-1, D1 * D2, R)
        embedded = jnp.einsum("npa,nad->npd", left, last, precision=high).reshape(-1, D1 * D2 * D3)
        pooled = jax.ops.segment_sum(embedded, bags, num_segments=BATCH_DEV)
        joined = jnp.concatenate([dense_block, pooled.astype(jnp.bfloat16)], axis=1)
        pre = jnp.dot(joined, w_top, preferred_element_type=jnp.float32) + bias_top[None, :]
        sig = jax.nn.sigmoid(pre)
        hidden = pre * sig
        logit = jnp.dot(hidden, w_out, precision=high)
        dlogit = (jax.nn.sigmoid(logit) - label_block.astype(jnp.float32)) / BATCH_DEV
        dpre = dlogit[:, None] * w_out[None, :] * (sig * (1.0 + pre * (1.0 - sig)))
        dpre_low = dpre.astype(jnp.bfloat16)
        grad_weight = jnp.dot(joined.T, dpre_low, preferred_element_type=jnp.float32)
        grad_bias = jnp.sum(dpre, axis=0)
        grad_output = jnp.sum(hidden * dlogit[:, None], axis=0)
        top_local = jnp.concatenate([grad_weight, grad_bias[None, :], grad_output[None, :]], axis=0)
        grad_pooled = jnp.dot(dpre_low, w_top[D1 * D2 * D3:].T, preferred_element_type=jnp.float32)
        grad_view = grad_pooled[bags].reshape(-1, D1 * D2, D3)
        grad_last = jnp.einsum("npa,npd->nad", left, grad_view, precision=high)
        grad_left = jnp.einsum("npd,nad->npa", grad_view, last, precision=high).reshape(-1, D1, D2 * R)
        grad_first = jnp.einsum("nib,nab->nia", grad_left, middle, precision=high)
        grad_middle = jnp.einsum("nia,nib->nab", first, grad_left, precision=high)
        sum_first = jax.ops.segment_sum(grad_first.reshape(-1, D1 * R), first_digit, num_segments=N1)
        sum_middle = jax.ops.segment_sum(grad_middle.reshape(-1, R * D2 * R), second_digit, num_segments=N2)
        sum_last = jax.ops.segment_sum(grad_last.reshape(-1, R * D3), third_digit, num_segments=N3)
        return (carry[0] + sum_first, carry[1] + sum_middle, carry[2] + sum_last, carry[3] + top_local), None

    start = (jnp.zeros((N1, D1 * R), jnp.float32), jnp.zeros((N2, R * D2 * R), jnp.float32),
             jnp.zeros((N3, R * D3), jnp.float32), jnp.zeros((2 * D1 * D2 * D3 + 2, HID), jnp.float32))
    totals, _ = lax.scan(device_terms, start, (dense_view, label_view, bag_ids, digit_one, digit_two, digit_three))
    core_grad = jnp.concatenate([totals[0].reshape(-1), totals[1].reshape(-1), totals[2].reshape(-1)])
    return core_grad, totals[3]
```

```python
import functools

import jax
import jax.numpy as jnp
from jax import lax
from jax.experimental import pallas as pl
from jax.experimental.pallas import tpu as pltpu
from jax.sharding import PartitionSpec as P

D1 = 4
D2 = 4
D3 = 8
R = 32
WIDTH = D1 * D2 * D3
PAIRS = D1 * D2
SIDE = D2 * R
AXES = ("gx", "gy")
F32 = jnp.float32
BF16 = jnp.bfloat16
HIGH = lax.Precision.HIGHEST


def dot(a, b, dims, precision=None):
    return lax.dot_general(
        a, b, (dims, ((), ())), precision=precision, preferred_element_type=F32
    )


def hot(row, count, kind):
    numbers = lax.broadcasted_iota(jnp.int32, (count, row.shape[1]), 0)
    return jnp.where(numbers == row, 1.0, 0.0).astype(kind)


def by_d3(last_t):
    size = R * D3
    to = lax.broadcasted_iota(jnp.int32, (size, size), 0)
    of = lax.broadcasted_iota(jnp.int32, (size, size), 1)
    turn = jnp.where(of == (to % R) * D3 + to // R, 1.0, 0.0).astype(BF16)
    return dot(turn, last_t, ((1,), (0,)))


def grad_left_into(gleft_s, g_s, lastd_s):
    @pl.loop(0, PAIRS)
    def _(p):
        total = None
        for d in range(D3):
            term = g_s[pl.ds(p * D3 + d, 1), :] * lastd_s[d * R:(d + 1) * R, :]
            total = term if total is None else total + term
        gleft_s[pl.ds(pl.multiple_of(p * R, R), R), :] = total


def local_kernel(
    c1, c2, c3, dense, w, bias, wout, labels, bag, d1, d2, d3,
    gp_ref, gw_ref, gv_ref, gf_ref, gl_ref,
    mid_s, first_s, last_s, lastd_s, left_s, gleft_s, emb_s, g_s, gf_s, gl_s,
):
    samples = dense.shape[0]
    looks = d1.shape[1]
    hot1 = hot(d1[...], c1.shape[0], BF16)
    hot2 = hot(d2[...], c2.shape[0], BF16)
    hot3 = hot(d3[...], c3.shape[0], BF16)
    down = ((0,), (0,))
    across = ((1,), (1,))
    plain = ((1,), (0,))
    for start in range(0, R * SIDE, 512):
        mid_s[start:start + 512, :] = dot(c2[:, start:start + 512], hot2, down)
    first_s[...] = dot(c1[...], hot1, down)
    last_t = dot(c3[...], hot3, down)
    last_s[...] = last_t
    lastd_s[...] = by_d3(last_t.astype(BF16))

    lane_blocks = looks // 128

    @pl.loop(0, D2 * lane_blocks)
    def _(step):
        j = step // lane_blocks
        lanes = pl.ds(pl.multiple_of((step % lane_blocks) * 128, 128), 128)
        totals = [None] * D1
        for a in range(R):
            m = mid_s[pl.ds(pl.multiple_of(a * SIDE + j * R, R), R), lanes]
            for i in range(D1):
                term = first_s[i * R + a:i * R + a + 1, lanes] * m
                totals[i] = term if totals[i] is None else totals[i] + term
        for i in range(D1):
            left_s[pl.ds(pl.multiple_of(i * SIDE + j * R, R), R), lanes] = totals[i]

    @pl.loop(0, PAIRS)
    def _(p):
        totals = [None, None]
        for c in range(R):
            term = left_s[pl.ds(p * R + c, 1), :] * last_s[c * D3:(c + 1) * D3, :]
            k = c % 2
            totals[k] = term if totals[k] is None else totals[k] + term
        emb_s[pl.ds(pl.multiple_of(p * D3, D3), D3), :] = totals[0] + totals[1]

    bags = hot(bag[...], samples, F32)
    pooled = dot(bags, emb_s[...], across, HIGH).astype(BF16)
    pre = (
        dot(dense[...], w[:WIDTH, :], plain) + dot(pooled, w[WIDTH:, :], plain)
        + bias[...]
    )
    sig = jax.nn.sigmoid(pre)
    hidden = pre * sig
    logit = jnp.sum(hidden * wout[...], axis=1, keepdims=True)
    rows = lax.broadcasted_iota(jnp.int32, (samples, samples), 0)
    cols = lax.broadcasted_iota(jnp.int32, (samples, samples), 1)
    label = jnp.sum(
        jnp.where(rows == cols, labels[...].astype(F32), 0.0), axis=1, keepdims=True
    )
    dlogit = (jax.nn.sigmoid(logit) - label) / samples
    dpre = dlogit * wout[...] * (sig * (1.0 + pre * (1.0 - sig)))
    low = dpre.astype(BF16)
    gw_ref[:WIDTH, :] = dot(dense[...], low, down)
    gw_ref[WIDTH:, :] = dot(pooled, low, down)
    gv_ref[0:1, :] = jnp.sum(dpre, axis=0, keepdims=True)
    gv_ref[1:2, :] = jnp.sum(hidden * dlogit, axis=0, keepdims=True)
    gp = dot(low, w[WIDTH:, :], across)
    gp_ref[...] = gp
    g_s[...] = dot(gp, bags, down, HIGH)

    grad_left_into(gleft_s, g_s, lastd_s)

    @pl.loop(0, R)
    def _(c):
        totals = [None, None]
        for p in range(PAIRS):
            term = left_s[pl.ds(p * R + c, 1), :] * g_s[p * D3:(p + 1) * D3, :]
            k = p % 2
            totals[k] = term if totals[k] is None else totals[k] + term
        gl_s[pl.ds(pl.multiple_of(c * D3, D3), D3), :] = totals[0] + totals[1]

    @pl.loop(0, R)
    def _(a):
        totals = [None] * D1
        for t in range(0, SIDE, 8):
            m = mid_s[pl.ds(pl.multiple_of(a * SIDE + t, 8), 8), :]
            for i in range(D1):
                term = gleft_s[i * SIDE + t:i * SIDE + t + 8, :] * m
                totals[i] = term if totals[i] is None else totals[i] + term
        for i in range(D1):
            gf_s[pl.ds(i * R + a, 1), :] = jnp.sum(totals[i], axis=0, keepdims=True)

    gf_ref[...] = dot(hot1.astype(F32), gf_s[...], across, HIGH)
    gl_ref[...] = dot(hot3.astype(F32), gl_s[...], across, HIGH)


def local_part(c1, c2, c3, dense, w, bias, wout, labels, bag, d1, d2, d3):
    samples, looks = dense.shape[0], d1.shape[1]
    shape = lambda *dims: jax.ShapeDtypeStruct(dims, F32)
    scratch = [R * SIDE, D1 * R, R * D3, R * D3, D1 * SIDE, D1 * SIDE, WIDTH, WIDTH, D1 * R, R * D3]
    return pl.pallas_call(
        local_kernel,
        out_shape=(
            shape(samples, WIDTH), shape(*w.shape), shape(2, w.shape[1]),
            shape(*c1.shape), shape(*c3.shape),
        ),
        scratch_shapes=[pltpu.VMEM((rows, looks), F32) for rows in scratch],
        compiler_params=pltpu.CompilerParams(vmem_limit_bytes=40 << 20),
        name="local",
    )(c1, c2, c3, dense, w, bias, wout, labels, bag, d1, d2, d3)


def middle_kernel(
    window, chunk, r0_ref, c1, c3, gp, digits, out_ref,
    rank_s, vals_s, g_s, lastd_s, gleft_s,
):
    groups, looks = digits.shape[1:]
    samples = gp.shape[0] // groups
    r0 = r0_ref[0]
    rel = digits[2] - r0
    inside = (rel >= 0) & (rel < window)
    mask = jnp.where(inside, 1.0, 0.0)
    low = mask.astype(BF16)
    tri = jnp.where(
        lax.broadcasted_iota(jnp.int32, (looks, looks), 0)
        < lax.broadcasted_iota(jnp.int32, (looks, looks), 1), 1.0, 0.0).astype(BF16)
    above = jnp.where(
        lax.broadcasted_iota(jnp.int32, (groups, groups), 0)
        > lax.broadcasted_iota(jnp.int32, (groups, groups), 1), 1.0, 0.0).astype(BF16)
    plain, across, down = ((1,), (0,)), ((1,), (1,)), ((0,), (0,))
    before = jnp.sum(dot(above, low, plain), axis=1, keepdims=True)
    rank_s[...] = jnp.where(inside, dot(low, tri, plain) + before, -1.0).astype(jnp.int32)
    count = jnp.sum(jnp.where(inside, 1, 0))
    group = lax.broadcasted_iota(jnp.int32, (groups, looks), 0)
    columns = (digits[0], digits[1], digits[3], group, jnp.where(inside, rel + 1, 0))
    for k, column in enumerate(columns):
        vals_s[:, k:k + 1, :] = column.astype(F32).reshape(groups, 1, looks)
    vals_s[:, len(columns):, :] = jnp.zeros((groups, 8 - len(columns), looks), F32)
    out_ref[...] = jnp.zeros_like(out_ref)
    gp_high = gp[...].astype(BF16)
    gp_low = (gp[...] - gp_high.astype(F32)).astype(BF16)
    slots = lax.broadcasted_iota(jnp.int32, (chunk, looks), 0)

    def body(step, carry):
        def pick(e, found):
            ranks = rank_s[pl.ds(e, 1), :] - step * chunk
            chosen = jnp.where(slots == ranks, 1.0, 0.0).astype(BF16)
            return found + dot(vals_s[e].astype(BF16), chosen, across)

        found = lax.fori_loop(0, groups, pick, jnp.zeros((8, chunk), F32), unroll=4)
        found = found.astype(jnp.int32)
        bag, d1, d3, owner, rel1 = (found[k:k + 1, :] for k in range(5))
        first = dot(c1[...], hot(d1, c1.shape[0], BF16), down)
        last = dot(c3[...], hot(d3, c3.shape[0], BF16), down)
        lastd_s[...] = by_d3(last.astype(BF16))
        sample = hot(owner * samples + bag, gp.shape[0], BF16)
        g_s[...] = dot(gp_high, sample, down) + dot(gp_low, sample, down)
        grad_left_into(gleft_s, g_s, lastd_s)
        total = out_ref[...]
        for i in range(D1):
            part = first[i * R:(i + 1) * R, :]
            spread = jnp.concatenate(
                [jnp.where(rel1 == r + 1, part, 0.0) for r in range(window)], axis=0
            ).astype(BF16)
            wide = gleft_s[i * SIDE:(i + 1) * SIDE, :]
            high = wide.astype(BF16)
            rest = (wide - high.astype(F32)).astype(BF16)
            total = total + dot(spread, high, across) + dot(spread, rest, across)
        out_ref[...] = total
        return carry

    lax.fori_loop(0, (count + chunk - 1) // chunk, body, 0)


def middle_part(window, r0, c1, c3, gp, digits):
    groups, looks = digits.shape[1:]
    chunk = 512
    vmem = pl.BlockSpec(memory_space=pltpu.VMEM)
    return pl.pallas_call(
        functools.partial(middle_kernel, window, chunk),
        out_shape=jax.ShapeDtypeStruct((window * R, SIDE), F32),
        in_specs=[pl.BlockSpec(memory_space=pltpu.SMEM), vmem, vmem, vmem, vmem],
        out_specs=vmem,
        scratch_shapes=[
            pltpu.VMEM((groups, looks), jnp.int32),
            pltpu.VMEM((groups, 8, looks), F32),
            pltpu.VMEM((WIDTH, chunk), F32),
            pltpu.VMEM((R * D3, chunk), F32),
            pltpu.VMEM((D1 * SIDE, chunk), F32),
        ],
        compiler_params=pltpu.CompilerParams(vmem_limit_bytes=40 << 20),
        name="middle",
    )(r0, c1, c3, gp, digits)


def cut(start, share, core_shapes, window, r0, first_sum, middle_rows, last_sum):
    n1 = core_shapes[0][0] * core_shapes[0][1]
    row = core_shapes[1][1]
    n2 = core_shapes[1][0] * row
    own_first = lax.dynamic_slice(
        jnp.pad(first_sum, (0, share)), (jnp.minimum(start, n1),), (share,))
    own_middle = lax.dynamic_slice(
        jnp.pad(middle_rows, (share, share)),
        (jnp.clip(start - n1 - r0 * row + share, 0, share + window * row),), (share,))
    own_last = lax.dynamic_slice(
        jnp.pad(last_sum, (share, 0)),
        (jnp.clip(start - n1 - n2 + share, 0, last_sum.shape[0]),), (share,))
    return own_first + own_middle + own_last


def per_device(devices, c1, c2, c3, dense, w, bias, wout, labels, bag, d1, d2, d3):
    total = c1.size + c2.size + c3.size
    share = total // devices
    row = c2.shape[1]
    window = min(-(-share // row) + 1, c2.shape[0])
    me = lax.axis_index(AXES)
    start = me * share
    r0 = jnp.clip((start - c1.size) // row, 0, c2.shape[0] - window)
    digits = lax.all_gather(jnp.stack([bag, d1, d2, d3]), AXES, axis=1, tiled=True)
    gp, gw, gv, gf, gl = local_part(
        c1, c2, c3, dense, w, bias[None], wout[None], labels[None], bag, d1, d2, d3)
    gp_all = lax.all_gather(gp, AXES, axis=0, tiled=True)
    gw, gv, gf, gl = lax.psum((gw, gv, gf, gl), AXES)
    rows = middle_part(window, r0[None], c1, c3, gp_all, digits)
    core = cut(start, share, (c1.shape, c2.shape, c3.shape), window, r0,
               gf.reshape(-1), rows.reshape(-1), gl.reshape(-1))
    return core, jnp.concatenate([gw, gv], axis=0)


def one_hot(digits, count, kind):
    return (digits[:, None] == jnp.arange(count, dtype=jnp.int32)[None, :]).astype(kind)


def slices(digits, core):
    return jnp.dot(
        one_hot(digits, core.shape[0], jnp.bfloat16), core, preferred_element_type=jnp.float32
    )


def factors(digits, cores):
    high = lax.Precision.HIGHEST
    first = slices(digits[0], cores[0]).reshape(-1, D1, R)
    middle = slices(digits[1], cores[1]).reshape(-1, R, D2 * R)
    last = slices(digits[2], cores[2]).reshape(-1, R, D3)
    left = jnp.einsum("nia,nab->nib", first, middle, precision=high).reshape(-1, D1 * D2, R)
    return (first, middle, last, left)


def top_total(top_local):
    return lax.psum(top_local, ("gx", "gy"))


def per_device_dense(
    core_one,
    core_two,
    core_three,
    dense_rows,
    w_top,
    bias_top,
    w_out,
    labels,
    bag_ids,
    digit_one,
    digit_two,
    digit_three,
):
    high = lax.Precision.HIGHEST
    cores = (core_one, core_two, core_three)
    digits = jnp.stack([digit_one[0], digit_two[0], digit_three[0]])
    looks = digits.shape[1]
    block = min(256, looks)
    blocks = looks // block
    blocked = digits.reshape(3, blocks, block).transpose(1, 0, 2)
    width = D1 * D2 * D3

    def forward(carry, part):
        first, middle, last, left = factors(part, cores)
        return (carry, jnp.einsum("npa,nad->npd", left, last, precision=high).reshape(block, width))

    _, embedded = lax.scan(forward, jnp.zeros((), jnp.float32), blocked)
    embedded = embedded.reshape(looks, width)
    samples = dense_rows.shape[0]
    bag_table = one_hot(bag_ids[0], samples, jnp.float32)
    pooled = jnp.dot(bag_table.T, embedded, precision=high)
    joined = jnp.concatenate([dense_rows, pooled.astype(jnp.bfloat16)], axis=1)
    pre = jnp.dot(joined, w_top, preferred_element_type=jnp.float32) + bias_top[None, :]
    sig = jax.nn.sigmoid(pre)
    hidden = pre * sig
    logit = jnp.dot(hidden, w_out, precision=high)
    dlogit = (jax.nn.sigmoid(logit) - labels.astype(jnp.float32)) / samples
    dpre = dlogit[:, None] * w_out[None, :] * (sig * (1.0 + pre * (1.0 - sig)))
    dpre_low = dpre.astype(jnp.bfloat16)
    grad_weight = jnp.dot(joined.T, dpre_low, preferred_element_type=jnp.float32)
    grad_bias = jnp.sum(dpre, axis=0)
    grad_output = jnp.sum(hidden * dlogit[:, None], axis=0)
    top_local = jnp.concatenate([grad_weight, grad_bias[None, :], grad_output[None, :]], axis=0)
    grad_pooled = jnp.dot(dpre_low, w_top[width:].T, preferred_element_type=jnp.float32)
    grad_embedded = jnp.dot(bag_table, grad_pooled, precision=high).reshape(blocks, block, width)

    def backward(totals, inputs):
        part, grad_block = inputs
        first, middle, last, left = factors(part, cores)
        grad_view = grad_block.reshape(block, D1 * D2, D3)
        grad_last = jnp.einsum("npa,npd->nad", left, grad_view, precision=high)
        grad_left = jnp.einsum("npd,nad->npa", grad_view, last, precision=high).reshape(
            block, D1, D2 * R
        )
        grad_first = jnp.einsum("nib,nab->nia", grad_left, middle, precision=high)
        grad_middle = jnp.einsum("nia,nib->nab", first, grad_left, precision=high)
        pieces = (
            grad_first.reshape(block, -1),
            grad_middle.reshape(block, -1),
            grad_last.reshape(block, -1),
        )
        updated = tuple(
            (
                total
                + jnp.dot(
                    one_hot(part[number], cores[number].shape[0], jnp.float32).T,
                    pieces[number],
                    precision=high,
                )
                for number, total in enumerate(totals)
            )
        )
        return (updated, None)

    start = tuple((jnp.zeros(core.shape, jnp.float32) for core in cores))
    totals, _ = lax.scan(backward, start, (blocked, grad_embedded))
    flat = jnp.concatenate([total.reshape(-1) for total in totals])
    core_grad = lax.psum_scatter(flat, ("gx", "gy"), scatter_dimension=0, tiled=True)
    top_grad = top_total(top_local)
    return (core_grad, top_grad)


def solution(mesh):
    devices = mesh.shape["gx"] * mesh.shape["gy"]
    whole, split, rows = P(), P(AXES), P(AXES, None)

    def step(*args):
        cores, dense = args[:3], args[3]
        if dense.size < sum(core.size for core in cores):
            body = functools.partial(per_device, devices)
        else:
            body = per_device_dense
        return jax.shard_map(
            body,
            mesh=mesh,
            in_specs=(
                whole, whole, whole, rows, whole, whole, whole, split,
                rows, rows, rows, rows,
            ),
            out_specs=(split, whole),
            check_vma=False,
        )(*args)

    return step
```

```python
import functools

import jax
import jax.numpy as jnp
from jax import lax
from jax.experimental import pallas as pl
from jax.experimental.pallas import tpu as pltpu
from jax.sharding import PartitionSpec as P

D1 = 4
D2 = 4
D3 = 8
R = 32
WIDTH = D1 * D2 * D3
PAIRS = D1 * D2
SIDE = D2 * R
AXES = ("gx", "gy")
F32 = jnp.float32
BF16 = jnp.bfloat16
HIGH = lax.Precision.HIGHEST


def dot(a, b, dims, precision=None):
    return lax.dot_general(
        a, b, (dims, ((), ())), precision=precision, preferred_element_type=F32
    )


def hot(row, count, kind):
    numbers = lax.broadcasted_iota(jnp.int32, (count, row.shape[1]), 0)
    return jnp.where(numbers == row, 1.0, 0.0).astype(kind)


def by_d3(last_t):
    size = R * D3
    to = lax.broadcasted_iota(jnp.int32, (size, size), 0)
    of = lax.broadcasted_iota(jnp.int32, (size, size), 1)
    turn = jnp.where(of == (to % R) * D3 + to // R, 1.0, 0.0).astype(BF16)
    return dot(turn, last_t, ((1,), (0,)))


def up(count, step):
    return -(-count // step) * step


def places_of(shape_one, shape_three, shape_top):
    places, at = {}, 0
    shapes = dict(
        weight=shape_top, first=shape_one, last=shape_three, vectors=(2, shape_top[1]))
    for name, (rows, columns) in shapes.items():
        places[name] = []
        for _ in range(columns // 128):
            places[name].append(at)
            at += up(rows, 8)
    return places, at


def grad_left_into(gleft_s, g_s, lastd_s):
    @pl.loop(0, PAIRS)
    def _(p):
        total = None
        for d in range(D3):
            term = g_s[pl.ds(p * D3 + d, 1), :] * lastd_s[d * R:(d + 1) * R, :]
            total = term if total is None else total + term
        gleft_s[pl.ds(pl.multiple_of(p * R, R), R), :] = total


def local_kernel(
    c1, c2, c3, dense, w, bias, wout, labels, bag, d1, d2, d3,
    block_ref, sums_ref,
    mid_s, first_s, last_s, lastd_s, left_s, gleft_s, emb_s, g_s, gf_s, gl_s,
):
    samples = dense.shape[0]
    looks = d1.shape[1]
    hot1 = hot(d1[...], c1.shape[0], BF16)
    hot2 = hot(d2[...], c2.shape[0], BF16)
    hot3 = hot(d3[...], c3.shape[0], BF16)
    down = ((0,), (0,))
    across = ((1,), (1,))
    plain = ((1,), (0,))
    for start in range(0, R * SIDE, 512):
        mid_s[start:start + 512, :] = dot(c2[:, start:start + 512], hot2, down)
    first_s[...] = dot(c1[...], hot1, down)
    last_t = dot(c3[...], hot3, down)
    last_s[...] = last_t
    lastd_s[...] = by_d3(last_t.astype(BF16))

    lane_blocks = looks // 128

    @pl.loop(0, D2 * lane_blocks)
    def _(step):
        j = step // lane_blocks
        lanes = pl.ds(pl.multiple_of((step % lane_blocks) * 128, 128), 128)
        totals = [None] * D1
        for a in range(R):
            m = mid_s[pl.ds(pl.multiple_of(a * SIDE + j * R, R), R), lanes]
            for i in range(D1):
                term = first_s[i * R + a:i * R + a + 1, lanes] * m
                totals[i] = term if totals[i] is None else totals[i] + term
        for i in range(D1):
            left_s[pl.ds(pl.multiple_of(i * SIDE + j * R, R), R), lanes] = totals[i]

    @pl.loop(0, PAIRS)
    def _(p):
        totals = [None, None]
        for c in range(R):
            term = left_s[pl.ds(p * R + c, 1), :] * last_s[c * D3:(c + 1) * D3, :]
            k = c % 2
            totals[k] = term if totals[k] is None else totals[k] + term
        emb_s[pl.ds(pl.multiple_of(p * D3, D3), D3), :] = totals[0] + totals[1]

    bags = hot(bag[...], samples, F32)
    pooled = dot(bags, emb_s[...], across, HIGH).astype(BF16)
    pre = (
        dot(dense[...], w[:WIDTH, :], plain) + dot(pooled, w[WIDTH:, :], plain)
        + bias[...]
    )
    sig = jax.nn.sigmoid(pre)
    hidden = pre * sig
    logit = jnp.sum(hidden * wout[...], axis=1, keepdims=True)
    rows = lax.broadcasted_iota(jnp.int32, (samples, samples), 0)
    cols = lax.broadcasted_iota(jnp.int32, (samples, samples), 1)
    label = jnp.sum(
        jnp.where(rows == cols, labels[...].astype(F32), 0.0), axis=1, keepdims=True
    )
    dlogit = (jax.nn.sigmoid(logit) - label) / samples
    dpre = dlogit * wout[...] * (sig * (1.0 + pre * (1.0 - sig)))
    low = dpre.astype(BF16)
    places, _ = places_of(c1.shape, c3.shape, w.shape)
    sums_ref[...] = jnp.zeros_like(sums_ref)

    def put(name, row, value):
        for h in range(value.shape[1] // 128):
            at = places[name][h] + row
            sums_ref[at:at + value.shape[0], :] = value[:, h * 128:(h + 1) * 128]

    put("weight", 0, dot(dense[...], low, down))
    put("weight", WIDTH, dot(pooled, low, down))
    put("vectors", 0, jnp.sum(dpre, axis=0, keepdims=True))
    put("vectors", 1, jnp.sum(hidden * dlogit, axis=0, keepdims=True))
    gp = dot(low, w[WIDTH:, :], across)
    block_ref[:samples, :] = gp
    block_ref[samples:, :] = jnp.zeros((block_ref.shape[0] - samples, 128), F32)
    for k, digit in enumerate((bag, d1, d2, d3)):
        for h in range(looks // 128):
            at = samples + k * (looks // 128) + h
            block_ref[at:at + 1, :] = digit[:, h * 128:(h + 1) * 128].astype(F32)
    g_s[...] = dot(gp, bags, down, HIGH)

    grad_left_into(gleft_s, g_s, lastd_s)

    @pl.loop(0, R)
    def _(c):
        totals = [None, None]
        for p in range(PAIRS):
            term = left_s[pl.ds(p * R + c, 1), :] * g_s[p * D3:(p + 1) * D3, :]
            k = p % 2
            totals[k] = term if totals[k] is None else totals[k] + term
        gl_s[pl.ds(pl.multiple_of(c * D3, D3), D3), :] = totals[0] + totals[1]

    @pl.loop(0, R)
    def _(a):
        totals = [None] * D1
        for t in range(0, SIDE, 8):
            m = mid_s[pl.ds(pl.multiple_of(a * SIDE + t, 8), 8), :]
            for i in range(D1):
                term = gleft_s[i * SIDE + t:i * SIDE + t + 8, :] * m
                totals[i] = term if totals[i] is None else totals[i] + term
        for i in range(D1):
            gf_s[pl.ds(i * R + a, 1), :] = jnp.sum(totals[i], axis=0, keepdims=True)

    put("first", 0, dot(hot1.astype(F32), gf_s[...], across, HIGH))
    put("last", 0, dot(hot3.astype(F32), gl_s[...], across, HIGH))


def local_part(devices, c1, c2, c3, dense, w, bias, wout, labels, bag, d1, d2, d3):
    samples, looks = dense.shape[0], d1.shape[1]
    shape = lambda *dims: jax.ShapeDtypeStruct(dims, F32)
    scratch = [R * SIDE, D1 * R, R * D3, R * D3, D1 * SIDE, D1 * SIDE, WIDTH, WIDTH, D1 * R, R * D3]
    return pl.pallas_call(
        local_kernel,
        out_shape=(
            shape(samples + up(4 * looks // 128, 8), WIDTH),
            shape(up(places_of(c1.shape, c3.shape, w.shape)[1], 8 * devices), 128),
        ),
        scratch_shapes=[pltpu.VMEM((rows, looks), F32) for rows in scratch],
        compiler_params=pltpu.CompilerParams(vmem_limit_bytes=40 << 20),
        name="local",
    )(c1, c2, c3, dense, w, bias, wout, labels, bag, d1, d2, d3)


def middle_kernel(
    window, chunk, samples, looks, r0_ref, c1, c3, blocks, out_ref,
    rank_s, vals_s, g_s, lastd_s, gleft_s,
):
    groups = blocks.shape[0]
    gp = blocks[:, :samples, :].reshape(groups * samples, WIDTH)
    per = looks // 128
    digits = [
        jnp.concatenate(
            [blocks[:, samples + k * per + h, :] for h in range(per)], axis=1
        ).astype(jnp.int32)
        for k in range(4)
    ]
    r0 = r0_ref[0]
    rel = digits[2] - r0
    inside = (rel >= 0) & (rel < window)
    mask = jnp.where(inside, 1.0, 0.0)
    low = mask.astype(BF16)
    tri = jnp.where(
        lax.broadcasted_iota(jnp.int32, (looks, looks), 0)
        < lax.broadcasted_iota(jnp.int32, (looks, looks), 1), 1.0, 0.0).astype(BF16)
    above = jnp.where(
        lax.broadcasted_iota(jnp.int32, (groups, groups), 0)
        > lax.broadcasted_iota(jnp.int32, (groups, groups), 1), 1.0, 0.0).astype(BF16)
    plain, across, down = ((1,), (0,)), ((1,), (1,)), ((0,), (0,))
    before = jnp.sum(dot(above, low, plain), axis=1, keepdims=True)
    rank_s[...] = jnp.where(inside, dot(low, tri, plain) + before, -1.0).astype(jnp.int32)
    count = jnp.sum(jnp.where(inside, 1, 0))
    group = lax.broadcasted_iota(jnp.int32, (groups, looks), 0)
    columns = (digits[0], digits[1], digits[3], group, jnp.where(inside, rel + 1, 0))
    for k, column in enumerate(columns):
        vals_s[:, k:k + 1, :] = column.astype(F32).reshape(groups, 1, looks)
    vals_s[:, len(columns):, :] = jnp.zeros((groups, 8 - len(columns), looks), F32)
    out_ref[...] = jnp.zeros_like(out_ref)
    gp_high = gp.astype(BF16)
    gp_low = (gp - gp_high.astype(F32)).astype(BF16)
    slots = lax.broadcasted_iota(jnp.int32, (chunk, looks), 0)

    def body(step, carry):
        def pick(e, found):
            ranks = rank_s[pl.ds(e, 1), :] - step * chunk
            chosen = jnp.where(slots == ranks, 1.0, 0.0).astype(BF16)
            return found + dot(vals_s[e].astype(BF16), chosen, across)

        found = lax.fori_loop(0, groups, pick, jnp.zeros((8, chunk), F32), unroll=4)
        found = found.astype(jnp.int32)
        bag, d1, d3, owner, rel1 = (found[k:k + 1, :] for k in range(5))
        first = dot(c1[...], hot(d1, c1.shape[0], BF16), down)
        last = dot(c3[...], hot(d3, c3.shape[0], BF16), down)
        lastd_s[...] = by_d3(last.astype(BF16))
        sample = hot(owner * samples + bag, gp.shape[0], BF16)
        g_s[...] = dot(gp_high, sample, down) + dot(gp_low, sample, down)
        grad_left_into(gleft_s, g_s, lastd_s)
        total = out_ref[...]
        for i in range(D1):
            part = first[i * R:(i + 1) * R, :]
            spread = jnp.concatenate(
                [jnp.where(rel1 == r + 1, part, 0.0) for r in range(window)], axis=0
            ).astype(BF16)
            wide = gleft_s[i * SIDE:(i + 1) * SIDE, :]
            high = wide.astype(BF16)
            rest = (wide - high.astype(F32)).astype(BF16)
            total = total + dot(spread, high, across) + dot(spread, rest, across)
        out_ref[...] = total
        return carry

    lax.fori_loop(0, (count + chunk - 1) // chunk, body, 0)


def middle_part(window, samples, looks, r0, c1, c3, blocks):
    groups = blocks.shape[0]
    chunk = 512
    vmem = pl.BlockSpec(memory_space=pltpu.VMEM)
    return pl.pallas_call(
        functools.partial(middle_kernel, window, chunk, samples, looks),
        out_shape=jax.ShapeDtypeStruct((window * R, SIDE), F32),
        in_specs=[pl.BlockSpec(memory_space=pltpu.SMEM), vmem, vmem, vmem],
        out_specs=vmem,
        scratch_shapes=[
            pltpu.VMEM((groups, looks), jnp.int32),
            pltpu.VMEM((groups, 8, looks), F32),
            pltpu.VMEM((WIDTH, chunk), F32),
            pltpu.VMEM((R * D3, chunk), F32),
            pltpu.VMEM((D1 * SIDE, chunk), F32),
        ],
        compiler_params=pltpu.CompilerParams(vmem_limit_bytes=40 << 20),
        name="middle",
    )(r0, c1, c3, blocks)


def exchange_kernel(
    nx, ny, block, sums, blocks_ref, total_ref,
    parts, send_a, recv_a, send_b, recv_b, send_c, recv_c,
):
    n = nx * ny
    me = lax.axis_index("gx") * ny + lax.axis_index("gy")

    def place(peer):
        return (peer // ny, peer % ny)

    def remote(src, dst, send, recv, peer):
        return pltpu.make_async_remote_copy(
            src_ref=src, dst_ref=dst, send_sem=send, recv_sem=recv,
            device_id=place(peer), device_id_type=pl.DeviceIdType.MESH)

    def part_copy(k, peer, slot):
        return remote(sums.at[peer], parts.at[slot], send_a.at[k], recv_a.at[slot], peer)

    def block_copy(k, peer, slot):
        return remote(block, blocks_ref.at[slot], send_b.at[k], recv_b.at[slot], peer)

    def total_copy(k, peer, slot):
        return remote(
            total_ref.at[me], total_ref.at[slot], send_c.at[k], recv_c.at[slot], peer)

    def peers(body):
        @pl.loop(1, n)
        def _(k):
            body(k, lax.rem(me + k, n))

    barrier = pltpu.get_barrier_semaphore()
    peers(lambda k, peer: pl.semaphore_signal(
        barrier, inc=1, device_id=place(peer), device_id_type=pl.DeviceIdType.MESH))
    pl.semaphore_wait(barrier, n - 1)

    peers(lambda k, peer: part_copy(k, peer, me).start())
    peers(lambda k, peer: block_copy(k, peer, me).start())
    blocks_ref[me] = block[...]

    def add(k, total):
        peer = lax.rem(me + k, n)
        part_copy(k, peer, peer).wait_recv()
        return total + parts[peer]

    total_ref[me] = lax.fori_loop(1, n, add, sums[me])
    peers(lambda k, peer: total_copy(k, peer, me).start())
    peers(lambda k, peer: block_copy(k, peer, peer).wait_recv())
    peers(lambda k, peer: total_copy(k, peer, peer).wait_recv())
    peers(lambda k, peer: part_copy(k, peer, me).wait_send())
    peers(lambda k, peer: block_copy(k, peer, me).wait_send())
    peers(lambda k, peer: total_copy(k, peer, me).wait_send())


def exchange(nx, ny, block, sums):
    n = nx * ny
    part = sums.shape[0] // n
    vmem = pl.BlockSpec(memory_space=pltpu.VMEM)
    return pl.pallas_call(
        functools.partial(exchange_kernel, nx, ny),
        out_shape=(
            jax.ShapeDtypeStruct((n, *block.shape), F32),
            jax.ShapeDtypeStruct((n, part, 128), F32),
        ),
        in_specs=[vmem, vmem],
        out_specs=(vmem, vmem),
        scratch_shapes=[pltpu.VMEM((n, part, 128), F32)]
        + [pltpu.SemaphoreType.DMA((n,))] * 6,
        compiler_params=pltpu.CompilerParams(
            collective_id=0, has_side_effects=True, vmem_limit_bytes=24 << 20),
        name="exchange",
    )(block, sums.reshape(n, part, 128))


def cut(start, share, core_shapes, window, r0, first_sum, middle_rows, last_sum):
    n1 = core_shapes[0][0] * core_shapes[0][1]
    row = core_shapes[1][1]
    n2 = core_shapes[1][0] * row
    own_first = lax.dynamic_slice(
        jnp.pad(first_sum, (0, share)), (jnp.minimum(start, n1),), (share,))
    own_middle = lax.dynamic_slice(
        jnp.pad(middle_rows, (share, share)),
        (jnp.clip(start - n1 - r0 * row + share, 0, share + window * row),), (share,))
    own_last = lax.dynamic_slice(
        jnp.pad(last_sum, (share, 0)),
        (jnp.clip(start - n1 - n2 + share, 0, last_sum.shape[0]),), (share,))
    return own_first + own_middle + own_last


def per_device(nx, ny, c1, c2, c3, dense, w, bias, wout, labels, bag, d1, d2, d3):
    devices = nx * ny
    total = c1.size + c2.size + c3.size
    share = total // devices
    row = c2.shape[1]
    window = min(-(-share // row) + 1, c2.shape[0])
    start = (lax.axis_index("gx") * ny + lax.axis_index("gy")) * share
    r0 = jnp.clip((start - c1.size) // row, 0, c2.shape[0] - window)
    block, sums = local_part(
        devices, c1, c2, c3, dense, w, bias[None], wout[None], labels[None], bag, d1, d2, d3)
    blocks, sums = exchange(nx, ny, block, sums)
    rows = middle_part(window, dense.shape[0], d1.shape[1], r0[None], c1, c3, blocks)
    sums = sums.reshape(-1, 128)
    places, _ = places_of(c1.shape, c3.shape, w.shape)

    def take(name, count):
        return jnp.concatenate([sums[at:at + count] for at in places[name]], axis=1)

    core = cut(start, share, (c1.shape, c2.shape, c3.shape), window, r0,
               take("first", c1.shape[0]).reshape(-1), rows.reshape(-1),
               take("last", c3.shape[0]).reshape(-1))
    return core, jnp.concatenate([take("weight", w.shape[0]), take("vectors", 2)], axis=0)


def one_hot(digits, count, kind):
    return (digits[:, None] == jnp.arange(count, dtype=jnp.int32)[None, :]).astype(kind)


def slices(digits, core):
    return jnp.dot(
        one_hot(digits, core.shape[0], jnp.bfloat16), core, preferred_element_type=jnp.float32
    )


def factors(digits, cores):
    high = lax.Precision.HIGHEST
    first = slices(digits[0], cores[0]).reshape(-1, D1, R)
    middle = slices(digits[1], cores[1]).reshape(-1, R, D2 * R)
    last = slices(digits[2], cores[2]).reshape(-1, R, D3)
    left = jnp.einsum("nia,nab->nib", first, middle, precision=high).reshape(-1, D1 * D2, R)
    return (first, middle, last, left)


def top_total(top_local):
    return lax.psum(top_local, ("gx", "gy"))


def per_device_dense(
    core_one,
    core_two,
    core_three,
    dense_rows,
    w_top,
    bias_top,
    w_out,
    labels,
    bag_ids,
    digit_one,
    digit_two,
    digit_three,
):
    high = lax.Precision.HIGHEST
    cores = (core_one, core_two, core_three)
    digits = jnp.stack([digit_one[0], digit_two[0], digit_three[0]])
    looks = digits.shape[1]
    block = min(256, looks)
    blocks = looks // block
    blocked = digits.reshape(3, blocks, block).transpose(1, 0, 2)
    width = D1 * D2 * D3

    def forward(carry, part):
        first, middle, last, left = factors(part, cores)
        return (carry, jnp.einsum("npa,nad->npd", left, last, precision=high).reshape(block, width))

    _, embedded = lax.scan(forward, jnp.zeros((), jnp.float32), blocked)
    embedded = embedded.reshape(looks, width)
    samples = dense_rows.shape[0]
    bag_table = one_hot(bag_ids[0], samples, jnp.float32)
    pooled = jnp.dot(bag_table.T, embedded, precision=high)
    joined = jnp.concatenate([dense_rows, pooled.astype(jnp.bfloat16)], axis=1)
    pre = jnp.dot(joined, w_top, preferred_element_type=jnp.float32) + bias_top[None, :]
    sig = jax.nn.sigmoid(pre)
    hidden = pre * sig
    logit = jnp.dot(hidden, w_out, precision=high)
    dlogit = (jax.nn.sigmoid(logit) - labels.astype(jnp.float32)) / samples
    dpre = dlogit[:, None] * w_out[None, :] * (sig * (1.0 + pre * (1.0 - sig)))
    dpre_low = dpre.astype(jnp.bfloat16)
    grad_weight = jnp.dot(joined.T, dpre_low, preferred_element_type=jnp.float32)
    grad_bias = jnp.sum(dpre, axis=0)
    grad_output = jnp.sum(hidden * dlogit[:, None], axis=0)
    top_local = jnp.concatenate([grad_weight, grad_bias[None, :], grad_output[None, :]], axis=0)
    grad_pooled = jnp.dot(dpre_low, w_top[width:].T, preferred_element_type=jnp.float32)
    grad_embedded = jnp.dot(bag_table, grad_pooled, precision=high).reshape(blocks, block, width)

    def backward(totals, inputs):
        part, grad_block = inputs
        first, middle, last, left = factors(part, cores)
        grad_view = grad_block.reshape(block, D1 * D2, D3)
        grad_last = jnp.einsum("npa,npd->nad", left, grad_view, precision=high)
        grad_left = jnp.einsum("npd,nad->npa", grad_view, last, precision=high).reshape(
            block, D1, D2 * R
        )
        grad_first = jnp.einsum("nib,nab->nia", grad_left, middle, precision=high)
        grad_middle = jnp.einsum("nia,nib->nab", first, grad_left, precision=high)
        pieces = (
            grad_first.reshape(block, -1),
            grad_middle.reshape(block, -1),
            grad_last.reshape(block, -1),
        )
        updated = tuple(
            (
                total
                + jnp.dot(
                    one_hot(part[number], cores[number].shape[0], jnp.float32).T,
                    pieces[number],
                    precision=high,
                )
                for number, total in enumerate(totals)
            )
        )
        return (updated, None)

    start = tuple((jnp.zeros(core.shape, jnp.float32) for core in cores))
    totals, _ = lax.scan(backward, start, (blocked, grad_embedded))
    flat = jnp.concatenate([total.reshape(-1) for total in totals])
    core_grad = lax.psum_scatter(flat, ("gx", "gy"), scatter_dimension=0, tiled=True)
    top_grad = top_total(top_local)
    return (core_grad, top_grad)


def solution(mesh):
    nx, ny = mesh.shape["gx"], mesh.shape["gy"]
    whole, split, rows = P(), P(AXES), P(AXES, None)

    def step(*args):
        cores, dense = args[:3], args[3]
        if dense.size < sum(core.size for core in cores):
            body = functools.partial(per_device, nx, ny)
        else:
            body = per_device_dense
        return jax.shard_map(
            body,
            mesh=mesh,
            in_specs=(
                whole, whole, whole, rows, whole, whole, whole, split,
                rows, rows, rows, rows,
            ),
            out_specs=(split, whole),
            check_vma=False,
        )(*args)

    return step
```

```python
import functools

import jax
import jax.numpy as jnp
from jax import lax
from jax.experimental import pallas as pl
from jax.experimental.pallas import tpu as pltpu
from jax.sharding import PartitionSpec as P

D1 = 4
D2 = 4
D3 = 8
R = 32
WIDTH = D1 * D2 * D3
PAIRS = D1 * D2
SIDE = D2 * R
AXES = ("gx", "gy")
F32 = jnp.float32
BF16 = jnp.bfloat16
HIGH = lax.Precision.HIGHEST


def dot(a, b, dims, precision=None):
    return lax.dot_general(
        a, b, (dims, ((), ())), precision=precision, preferred_element_type=F32
    )


def hot(row, count, kind):
    numbers = lax.broadcasted_iota(jnp.int32, (count, row.shape[1]), 0)
    return jnp.where(numbers == row, 1.0, 0.0).astype(kind)


def by_d3(last_t):
    size = R * D3
    to = lax.broadcasted_iota(jnp.int32, (size, size), 0)
    of = lax.broadcasted_iota(jnp.int32, (size, size), 1)
    turn = jnp.where(of == (to % R) * D3 + to // R, 1.0, 0.0).astype(BF16)
    return dot(turn, last_t, ((1,), (0,)))


def up(count, step):
    return -(-count // step) * step


def places_of(shape_one, shape_three, shape_top):
    places, at = {}, 0
    shapes = dict(
        weight=shape_top, first=shape_one, last=shape_three, vectors=(2, shape_top[1]))
    for name, (rows, columns) in shapes.items():
        places[name] = []
        for _ in range(columns // 128):
            places[name].append(at)
            at += up(rows, 8)
    return places, at


def grad_left_into(gleft_s, g_s, lastd_s):
    @pl.loop(0, PAIRS)
    def _(p):
        total = None
        for d in range(D3):
            term = g_s[pl.ds(p * D3 + d, 1), :] * lastd_s[d * R:(d + 1) * R, :]
            total = term if total is None else total + term
        gleft_s[pl.ds(pl.multiple_of(p * R, R), R), :] = total


def local_kernel(
    c1, c2, c3, dense, w, bias, wout, labels, bag, d1, d2, d3,
    block_ref, sums_ref,
    mid_s, first_s, last_s, lastd_s, left_s, gleft_s, emb_s, g_s, gf_s, gl_s,
):
    samples = dense.shape[0]
    looks = d1.shape[1]
    hot1 = hot(d1[...], c1.shape[0], BF16)
    hot2 = hot(d2[...], c2.shape[0], BF16)
    hot3 = hot(d3[...], c3.shape[0], BF16)
    down = ((0,), (0,))
    across = ((1,), (1,))
    plain = ((1,), (0,))
    for start in range(0, R * SIDE, 512):
        mid_s[start:start + 512, :] = dot(c2[:, start:start + 512], hot2, down)
    first_s[...] = dot(c1[...], hot1, down)
    last_t = dot(c3[...], hot3, down)
    last_s[...] = last_t
    lastd_s[...] = by_d3(last_t.astype(BF16))

    lane_blocks = looks // 128

    @pl.loop(0, D2 * lane_blocks)
    def _(step):
        j = step // lane_blocks
        lanes = pl.ds(pl.multiple_of((step % lane_blocks) * 128, 128), 128)
        totals = [None] * D1
        for a in range(R):
            m = mid_s[pl.ds(pl.multiple_of(a * SIDE + j * R, R), R), lanes]
            for i in range(D1):
                term = first_s[i * R + a:i * R + a + 1, lanes] * m
                totals[i] = term if totals[i] is None else totals[i] + term
        for i in range(D1):
            left_s[pl.ds(pl.multiple_of(i * SIDE + j * R, R), R), lanes] = totals[i]

    @pl.loop(0, PAIRS)
    def _(p):
        totals = [None, None]
        for c in range(R):
            term = left_s[pl.ds(p * R + c, 1), :] * last_s[c * D3:(c + 1) * D3, :]
            k = c % 2
            totals[k] = term if totals[k] is None else totals[k] + term
        emb_s[pl.ds(pl.multiple_of(p * D3, D3), D3), :] = totals[0] + totals[1]

    bags = hot(bag[...], samples, F32)
    pooled = dot(bags, emb_s[...], across, HIGH).astype(BF16)
    pre = (
        dot(dense[...], w[:WIDTH, :], plain) + dot(pooled, w[WIDTH:, :], plain)
        + bias[...]
    )
    sig = jax.nn.sigmoid(pre)
    hidden = pre * sig
    logit = jnp.sum(hidden * wout[...], axis=1, keepdims=True)
    rows = lax.broadcasted_iota(jnp.int32, (samples, samples), 0)
    cols = lax.broadcasted_iota(jnp.int32, (samples, samples), 1)
    label = jnp.sum(
        jnp.where(rows == cols, labels[...].astype(F32), 0.0), axis=1, keepdims=True
    )
    dlogit = (jax.nn.sigmoid(logit) - label) / samples
    dpre = dlogit * wout[...] * (sig * (1.0 + pre * (1.0 - sig)))
    low = dpre.astype(BF16)
    places, _ = places_of(c1.shape, c3.shape, w.shape)
    sums_ref[...] = jnp.zeros_like(sums_ref)

    def put(name, row, value):
        for h in range(value.shape[1] // 128):
            at = places[name][h] + row
            sums_ref[at:at + value.shape[0], :] = value[:, h * 128:(h + 1) * 128]

    put("weight", 0, dot(dense[...], low, down))
    put("weight", WIDTH, dot(pooled, low, down))
    put("vectors", 0, jnp.sum(dpre, axis=0, keepdims=True))
    put("vectors", 1, jnp.sum(hidden * dlogit, axis=0, keepdims=True))
    gp = dot(low, w[WIDTH:, :], across)
    block_ref[:samples, :] = gp
    block_ref[samples:, :] = jnp.zeros((block_ref.shape[0] - samples, 128), F32)
    for k, digit in enumerate((bag, d1, d2, d3)):
        for h in range(looks // 128):
            at = samples + k * (looks // 128) + h
            block_ref[at:at + 1, :] = digit[:, h * 128:(h + 1) * 128].astype(F32)
    g_s[...] = dot(gp, bags, down, HIGH)

    grad_left_into(gleft_s, g_s, lastd_s)

    @pl.loop(0, R)
    def _(c):
        totals = [None, None]
        for p in range(PAIRS):
            term = left_s[pl.ds(p * R + c, 1), :] * g_s[p * D3:(p + 1) * D3, :]
            k = p % 2
            totals[k] = term if totals[k] is None else totals[k] + term
        gl_s[pl.ds(pl.multiple_of(c * D3, D3), D3), :] = totals[0] + totals[1]

    @pl.loop(0, R)
    def _(a):
        totals = [None] * D1
        for t in range(0, SIDE, 8):
            m = mid_s[pl.ds(pl.multiple_of(a * SIDE + t, 8), 8), :]
            for i in range(D1):
                term = gleft_s[i * SIDE + t:i * SIDE + t + 8, :] * m
                totals[i] = term if totals[i] is None else totals[i] + term
        for i in range(D1):
            gf_s[pl.ds(i * R + a, 1), :] = jnp.sum(totals[i], axis=0, keepdims=True)

    put("first", 0, dot(hot1.astype(F32), gf_s[...], across, HIGH))
    put("last", 0, dot(hot3.astype(F32), gl_s[...], across, HIGH))


def fetch_then(count, kernel, *refs):
    inputs, rest = refs[:count], refs[count:-count - 1]
    held, sems = refs[-count - 1:-1], refs[-1]
    copies = [
        pltpu.make_async_copy(inputs[k], held[k], sems.at[k]) for k in range(count)]
    for copy in copies:
        copy.start()
    for copy in copies:
        copy.wait()
    kernel(*held, *rest)


def local_part(devices, c1, c2, c3, dense, w, bias, wout, labels, bag, d1, d2, d3):
    samples, looks = dense.shape[0], d1.shape[1]
    shape = lambda *dims: jax.ShapeDtypeStruct(dims, F32)
    scratch = [R * SIDE, D1 * R, R * D3, R * D3, D1 * SIDE, D1 * SIDE, WIDTH, WIDTH, D1 * R, R * D3]
    inputs = (c1, c2, c3, dense, w, bias, wout, labels, bag, d1, d2, d3)
    return pl.pallas_call(
        functools.partial(fetch_then, len(inputs), local_kernel),
        in_specs=[pl.BlockSpec(memory_space=pltpu.HBM)] * len(inputs),
        out_shape=(
            shape(samples + up(4 * looks // 128, 8), WIDTH),
            shape(up(places_of(c1.shape, c3.shape, w.shape)[1], 8 * devices), 128),
        ),
        scratch_shapes=[pltpu.VMEM((rows, looks), F32) for rows in scratch]
        + [pltpu.VMEM(x.shape, x.dtype) for x in inputs]
        + [pltpu.SemaphoreType.DMA((len(inputs),))],
        compiler_params=pltpu.CompilerParams(vmem_limit_bytes=40 << 20),
        name="local",
    )(*inputs)


def middle_kernel(
    window, chunk, samples, looks, r0_ref, c1, c3, blocks, out_ref,
    rank_s, vals_s, g_s, lastd_s, gleft_s,
):
    groups = blocks.shape[0]
    gp = blocks[:, :samples, :].reshape(groups * samples, WIDTH)
    per = looks // 128
    digits = [
        jnp.concatenate(
            [blocks[:, samples + k * per + h, :] for h in range(per)], axis=1
        ).astype(jnp.int32)
        for k in range(4)
    ]
    r0 = r0_ref[0]
    rel = digits[2] - r0
    inside = (rel >= 0) & (rel < window)
    mask = jnp.where(inside, 1.0, 0.0)
    low = mask.astype(BF16)
    tri = jnp.where(
        lax.broadcasted_iota(jnp.int32, (looks, looks), 0)
        < lax.broadcasted_iota(jnp.int32, (looks, looks), 1), 1.0, 0.0).astype(BF16)
    above = jnp.where(
        lax.broadcasted_iota(jnp.int32, (groups, groups), 0)
        > lax.broadcasted_iota(jnp.int32, (groups, groups), 1), 1.0, 0.0).astype(BF16)
    plain, across, down = ((1,), (0,)), ((1,), (1,)), ((0,), (0,))
    before = jnp.sum(dot(above, low, plain), axis=1, keepdims=True)
    rank_s[...] = jnp.where(inside, dot(low, tri, plain) + before, -1.0).astype(jnp.int32)
    count = jnp.sum(jnp.where(inside, 1, 0))
    group = lax.broadcasted_iota(jnp.int32, (groups, looks), 0)
    columns = (digits[0], digits[1], digits[3], group, jnp.where(inside, rel + 1, 0))
    for k, column in enumerate(columns):
        vals_s[:, k:k + 1, :] = column.astype(F32).reshape(groups, 1, looks)
    vals_s[:, len(columns):, :] = jnp.zeros((groups, 8 - len(columns), looks), F32)
    out_ref[...] = jnp.zeros_like(out_ref)
    gp_high = gp.astype(BF16)
    gp_low = (gp - gp_high.astype(F32)).astype(BF16)
    slots = lax.broadcasted_iota(jnp.int32, (chunk, looks), 0)

    def body(step, carry):
        def pick(e, found):
            ranks = rank_s[pl.ds(e, 1), :] - step * chunk
            chosen = jnp.where(slots == ranks, 1.0, 0.0).astype(BF16)
            return found + dot(vals_s[e].astype(BF16), chosen, across)

        found = lax.fori_loop(0, groups, pick, jnp.zeros((8, chunk), F32), unroll=4)
        found = found.astype(jnp.int32)
        bag, d1, d3, owner, rel1 = (found[k:k + 1, :] for k in range(5))
        first = dot(c1[...], hot(d1, c1.shape[0], BF16), down)
        last = dot(c3[...], hot(d3, c3.shape[0], BF16), down)
        lastd_s[...] = by_d3(last.astype(BF16))
        sample = hot(owner * samples + bag, gp.shape[0], BF16)
        g_s[...] = dot(gp_high, sample, down) + dot(gp_low, sample, down)
        grad_left_into(gleft_s, g_s, lastd_s)
        total = out_ref[...]
        for i in range(D1):
            part = first[i * R:(i + 1) * R, :]
            spread = jnp.concatenate(
                [jnp.where(rel1 == r + 1, part, 0.0) for r in range(window)], axis=0
            ).astype(BF16)
            wide = gleft_s[i * SIDE:(i + 1) * SIDE, :]
            high = wide.astype(BF16)
            rest = (wide - high.astype(F32)).astype(BF16)
            total = total + dot(spread, high, across) + dot(spread, rest, across)
        out_ref[...] = total
        return carry

    lax.fori_loop(0, (count + chunk - 1) // chunk, body, 0)


def middle_part(window, samples, looks, r0, c1, c3, blocks):
    groups = blocks.shape[0]
    chunk = 512
    vmem = pl.BlockSpec(memory_space=pltpu.VMEM)
    return pl.pallas_call(
        functools.partial(middle_kernel, window, chunk, samples, looks),
        out_shape=jax.ShapeDtypeStruct((window * R, SIDE), F32),
        in_specs=[pl.BlockSpec(memory_space=pltpu.SMEM), vmem, vmem, vmem],
        out_specs=vmem,
        scratch_shapes=[
            pltpu.VMEM((groups, looks), jnp.int32),
            pltpu.VMEM((groups, 8, looks), F32),
            pltpu.VMEM((WIDTH, chunk), F32),
            pltpu.VMEM((R * D3, chunk), F32),
            pltpu.VMEM((D1 * SIDE, chunk), F32),
        ],
        compiler_params=pltpu.CompilerParams(vmem_limit_bytes=40 << 20),
        name="middle",
    )(r0, c1, c3, blocks)


def levels(nx, ny):
    cores = 2 if nx % 2 == 0 else 1
    return cores, nx // cores, ny


def exchange_kernel(
    nx, ny, block, sums, blocks_ref, total_ref,
    part0, part1, part2, acc0, acc1, *sems,
):
    cores, chips, planes = levels(nx, ny)
    gx, plane = lax.axis_index("gx"), lax.axis_index("gy")
    core, chip = gx % cores, gx // cores

    def on_core(k):
        return (chip * cores + (core + k) % cores, plane)

    def on_chip(k):
        return (((chip + k) % chips) * cores + core, plane)

    def on_plane(k):
        return (gx, (plane + k) % planes)

    def remote(src, dst, number, k, peer):
        return pltpu.make_async_remote_copy(
            src_ref=src, dst_ref=dst,
            send_sem=sems[2 * number].at[k], recv_sem=sems[2 * number + 1].at[k],
            device_id=peer, device_id_type=pl.DeviceIdType.MESH)

    def stage(number, size, copy):
        for k in range(1, size):
            copy(k, k).start()

        def arrived():
            for k in range(1, size):
                copy(k, -k).wait_recv()

        def sent():
            for k in range(1, size):
                copy(k, k).wait_send()

        return arrived, sent

    def spread(ref, number, size, mine, view, peer):
        def copy(k, off):
            at = mine if off > 0 else (mine + off + size) % size
            return remote(view(ref, at), view(ref, at), number, k, peer(k))
        return stage(number, size, copy)

    barrier = pltpu.get_barrier_semaphore()
    greeted = 0
    for size, peer in ((cores, on_core), (chips, on_chip), (planes, on_plane)):
        for k in range(1, size):
            pl.semaphore_signal(
                barrier, inc=1, device_id=peer(k), device_id_type=pl.DeviceIdType.MESH)
            greeted += 1
    pl.semaphore_wait(barrier, greeted)

    sent = []

    def go(pair):
        sent.append(pair[1])
        return pair[0]

    def block_copy(k, off):
        at = plane if off > 0 else (plane + off + planes) % planes
        return remote(block, blocks_ref.at[core, chip, at], 3, k, on_plane(k))

    arrived_r0 = go(stage(0, cores, lambda k, off: remote(
        sums.at[(core + k) % cores], part0.at[k], 0, k, on_core(k))))
    arrived_bz = go(stage(3, planes, block_copy))
    blocks_ref[core, chip, plane] = block[...]

    arrived_r0()
    total = sums[core]
    for k in range(1, cores):
        total = total + part0[k]
    acc0[...] = total
    arrived_r1 = go(stage(1, chips, lambda k, off: remote(
        acc0.at[(chip + k) % chips], part1.at[k], 1, k, on_chip(k))))
    arrived_bz()
    arrived_b1 = go(spread(
        blocks_ref, 4, chips, chip, lambda r, at: r.at[core, at], on_chip))

    arrived_r1()
    total = acc0[chip]
    for k in range(1, chips):
        total = total + part1[k]
    acc1[...] = total
    arrived_r2 = go(stage(2, planes, lambda k, off: remote(
        acc1.at[(plane + k) % planes], part2.at[k], 2, k, on_plane(k))))
    arrived_r2()
    total = acc1[plane]
    for k in range(1, planes):
        total = total + part2[k]
    total_ref[core, chip, plane] = total
    go(spread(
        total_ref, 5, planes, plane, lambda r, at: r.at[core, chip, at], on_plane))()
    arrived_a1 = go(spread(
        total_ref, 6, chips, chip, lambda r, at: r.at[core, at], on_chip))
    arrived_b1()
    arrived_b0 = go(spread(blocks_ref, 7, cores, core, lambda r, at: r.at[at], on_core))
    arrived_a1()
    arrived_a0 = go(spread(total_ref, 8, cores, core, lambda r, at: r.at[at], on_core))
    arrived_b0()
    arrived_a0()
    for wait in sent:
        wait()


def exchange(nx, ny, block, sums):
    cores, chips, planes = levels(nx, ny)
    part = sums.shape[0] // (nx * ny)
    vmem = pl.BlockSpec(memory_space=pltpu.VMEM)
    shape = (cores, chips, planes, part, 128)
    scratch = [
        (cores, *shape[1:]), (chips, *shape[2:]), (planes, *shape[3:]), shape[1:], shape[2:]]
    sizes = (cores, chips, planes, planes, chips, planes, chips, cores, cores)
    blocks, total = pl.pallas_call(
        functools.partial(exchange_kernel, nx, ny),
        out_shape=(
            jax.ShapeDtypeStruct((cores, chips, planes, *block.shape), F32),
            jax.ShapeDtypeStruct(shape, F32),
        ),
        in_specs=[vmem, vmem],
        out_specs=(vmem, vmem),
        scratch_shapes=[pltpu.VMEM(dims, F32) for dims in scratch]
        + [pltpu.SemaphoreType.DMA((size,)) for size in sizes for _ in range(2)],
        compiler_params=pltpu.CompilerParams(
            collective_id=0, has_side_effects=True, vmem_limit_bytes=24 << 20),
        name="exchange",
    )(block, sums.reshape(shape))
    return blocks.reshape(-1, *block.shape), total


def cut(start, share, core_shapes, window, r0, first_sum, middle_rows, last_sum):
    n1 = core_shapes[0][0] * core_shapes[0][1]
    row = core_shapes[1][1]
    n2 = core_shapes[1][0] * row
    own_first = lax.dynamic_slice(
        jnp.pad(first_sum, (0, share)), (jnp.minimum(start, n1),), (share,))
    own_middle = lax.dynamic_slice(
        jnp.pad(middle_rows, (share, share)),
        (jnp.clip(start - n1 - r0 * row + share, 0, share + window * row),), (share,))
    own_last = lax.dynamic_slice(
        jnp.pad(last_sum, (share, 0)),
        (jnp.clip(start - n1 - n2 + share, 0, last_sum.shape[0]),), (share,))
    return own_first + own_middle + own_last


def per_device(nx, ny, c1, c2, c3, dense, w, bias, wout, labels, bag, d1, d2, d3):
    devices = nx * ny
    total = c1.size + c2.size + c3.size
    share = total // devices
    row = c2.shape[1]
    window = min(-(-share // row) + 1, c2.shape[0])
    start = (lax.axis_index("gx") * ny + lax.axis_index("gy")) * share
    r0 = jnp.clip((start - c1.size) // row, 0, c2.shape[0] - window)
    block, sums = local_part(
        devices, c1, c2, c3, dense, w, bias[None], wout[None], labels[None], bag, d1, d2, d3)
    blocks, sums = exchange(nx, ny, block, sums)
    rows = middle_part(window, dense.shape[0], d1.shape[1], r0[None], c1, c3, blocks)
    sums = sums.reshape(-1, 128)
    places, _ = places_of(c1.shape, c3.shape, w.shape)

    def take(name, count):
        return jnp.concatenate([sums[at:at + count] for at in places[name]], axis=1)

    core = cut(start, share, (c1.shape, c2.shape, c3.shape), window, r0,
               take("first", c1.shape[0]).reshape(-1), rows.reshape(-1),
               take("last", c3.shape[0]).reshape(-1))
    return core, jnp.concatenate([take("weight", w.shape[0]), take("vectors", 2)], axis=0)


def one_hot(digits, count, kind):
    return (digits[:, None] == jnp.arange(count, dtype=jnp.int32)[None, :]).astype(kind)


def slices(digits, core):
    return jnp.dot(
        one_hot(digits, core.shape[0], jnp.bfloat16), core, preferred_element_type=jnp.float32
    )


def factors(digits, cores):
    high = lax.Precision.HIGHEST
    first = slices(digits[0], cores[0]).reshape(-1, D1, R)
    middle = slices(digits[1], cores[1]).reshape(-1, R, D2 * R)
    last = slices(digits[2], cores[2]).reshape(-1, R, D3)
    left = jnp.einsum("nia,nab->nib", first, middle, precision=high).reshape(-1, D1 * D2, R)
    return (first, middle, last, left)


def top_total(top_local):
    return lax.psum(top_local, ("gx", "gy"))


def per_device_dense(
    core_one,
    core_two,
    core_three,
    dense_rows,
    w_top,
    bias_top,
    w_out,
    labels,
    bag_ids,
    digit_one,
    digit_two,
    digit_three,
):
    high = lax.Precision.HIGHEST
    cores = (core_one, core_two, core_three)
    digits = jnp.stack([digit_one[0], digit_two[0], digit_three[0]])
    looks = digits.shape[1]
    block = min(256, looks)
    blocks = looks // block
    blocked = digits.reshape(3, blocks, block).transpose(1, 0, 2)
    width = D1 * D2 * D3

    def forward(carry, part):
        first, middle, last, left = factors(part, cores)
        return (carry, jnp.einsum("npa,nad->npd", left, last, precision=high).reshape(block, width))

    _, embedded = lax.scan(forward, jnp.zeros((), jnp.float32), blocked)
    embedded = embedded.reshape(looks, width)
    samples = dense_rows.shape[0]
    bag_table = one_hot(bag_ids[0], samples, jnp.float32)
    pooled = jnp.dot(bag_table.T, embedded, precision=high)
    joined = jnp.concatenate([dense_rows, pooled.astype(jnp.bfloat16)], axis=1)
    pre = jnp.dot(joined, w_top, preferred_element_type=jnp.float32) + bias_top[None, :]
    sig = jax.nn.sigmoid(pre)
    hidden = pre * sig
    logit = jnp.dot(hidden, w_out, precision=high)
    dlogit = (jax.nn.sigmoid(logit) - labels.astype(jnp.float32)) / samples
    dpre = dlogit[:, None] * w_out[None, :] * (sig * (1.0 + pre * (1.0 - sig)))
    dpre_low = dpre.astype(jnp.bfloat16)
    grad_weight = jnp.dot(joined.T, dpre_low, preferred_element_type=jnp.float32)
    grad_bias = jnp.sum(dpre, axis=0)
    grad_output = jnp.sum(hidden * dlogit[:, None], axis=0)
    top_local = jnp.concatenate([grad_weight, grad_bias[None, :], grad_output[None, :]], axis=0)
    grad_pooled = jnp.dot(dpre_low, w_top[width:].T, preferred_element_type=jnp.float32)
    grad_embedded = jnp.dot(bag_table, grad_pooled, precision=high).reshape(blocks, block, width)

    def backward(totals, inputs):
        part, grad_block = inputs
        first, middle, last, left = factors(part, cores)
        grad_view = grad_block.reshape(block, D1 * D2, D3)
        grad_last = jnp.einsum("npa,npd->nad", left, grad_view, precision=high)
        grad_left = jnp.einsum("npd,nad->npa", grad_view, last, precision=high).reshape(
            block, D1, D2 * R
        )
        grad_first = jnp.einsum("nib,nab->nia", grad_left, middle, precision=high)
        grad_middle = jnp.einsum("nia,nib->nab", first, grad_left, precision=high)
        pieces = (
            grad_first.reshape(block, -1),
            grad_middle.reshape(block, -1),
            grad_last.reshape(block, -1),
        )
        updated = tuple(
            (
                total
                + jnp.dot(
                    one_hot(part[number], cores[number].shape[0], jnp.float32).T,
                    pieces[number],
                    precision=high,
                )
                for number, total in enumerate(totals)
            )
        )
        return (updated, None)

    start = tuple((jnp.zeros(core.shape, jnp.float32) for core in cores))
    totals, _ = lax.scan(backward, start, (blocked, grad_embedded))
    flat = jnp.concatenate([total.reshape(-1) for total in totals])
    core_grad = lax.psum_scatter(flat, ("gx", "gy"), scatter_dimension=0, tiled=True)
    top_grad = top_total(top_local)
    return (core_grad, top_grad)


def solution(mesh):
    nx, ny = mesh.shape["gx"], mesh.shape["gy"]
    whole, split, rows = P(), P(AXES), P(AXES, None)

    def step(*args):
        cores, dense = args[:3], args[3]
        if dense.size < sum(core.size for core in cores):
            body = functools.partial(per_device, nx, ny)
        else:
            body = per_device_dense
        return jax.shard_map(
            body,
            mesh=mesh,
            in_specs=(
                whole, whole, whole, rows, whole, whole, whole, split,
                rows, rows, rows, rows,
            ),
            out_specs=(split, whole),
            check_vma=False,
        )(*args)

    return step
```

```python
import functools

import jax
import jax.numpy as jnp
from jax import lax
from jax.experimental import pallas as pl
from jax.experimental.pallas import tpu as pltpu
from jax.sharding import PartitionSpec as P

D1 = 4
D2 = 4
D3 = 8
R = 32
WIDTH = D1 * D2 * D3
PAIRS = D1 * D2
SIDE = D2 * R
AXES = ("gx", "gy")
F32 = jnp.float32
BF16 = jnp.bfloat16
HIGH = lax.Precision.HIGHEST


def dot(a, b, dims, precision=None):
    return lax.dot_general(
        a, b, (dims, ((), ())), precision=precision, preferred_element_type=F32
    )


def hot(row, count, kind):
    numbers = lax.broadcasted_iota(jnp.int32, (count, row.shape[1]), 0)
    return jnp.where(numbers == row, 1.0, 0.0).astype(kind)


def by_d3(last_t):
    size = R * D3
    to = lax.broadcasted_iota(jnp.int32, (size, size), 0)
    of = lax.broadcasted_iota(jnp.int32, (size, size), 1)
    turn = jnp.where(of == (to % R) * D3 + to // R, 1.0, 0.0).astype(BF16)
    return dot(turn, last_t, ((1,), (0,)))


def up(count, step):
    return -(-count // step) * step


def places_of(shape_one, shape_three, shape_top):
    places, at = {}, 0
    shapes = dict(
        weight=shape_top, first=shape_one, last=shape_three, vectors=(2, shape_top[1]))
    for name, (rows, columns) in shapes.items():
        places[name] = []
        for _ in range(columns // 128):
            places[name].append(at)
            at += up(rows, 8)
    return places, at


def grad_left_into(gleft_s, g_s, lastd_s):
    @pl.loop(0, PAIRS)
    def _(p):
        total = None
        for d in range(D3):
            term = g_s[pl.ds(p * D3 + d, 1), :] * lastd_s[d * R:(d + 1) * R, :]
            total = term if total is None else total + term
        gleft_s[pl.ds(pl.multiple_of(p * R, R), R), :] = total


def local_kernel(
    c1, c2, c3, dense, w, bias, wout, labels, bag, d1, d2, d3,
    block_ref, sums_ref,
    mid_s, first_s, last_s, lastd_s, left_s, gleft_s, emb_s, g_s, gf_s, gl_s,
):
    samples = dense.shape[0]
    looks = d1.shape[1]
    hot1 = hot(d1[...], c1.shape[0], BF16)
    hot2 = hot(d2[...], c2.shape[0], BF16)
    hot3 = hot(d3[...], c3.shape[0], BF16)
    down = ((0,), (0,))
    across = ((1,), (1,))
    plain = ((1,), (0,))
    for start in range(0, R * SIDE, 512):
        mid_s[start:start + 512, :] = dot(c2[:, start:start + 512], hot2, down)
    first_s[...] = dot(c1[...], hot1, down)
    last_t = dot(c3[...], hot3, down)
    last_s[...] = last_t
    lastd_s[...] = by_d3(last_t.astype(BF16))

    lane_blocks = looks // 128

    @pl.loop(0, D2 * lane_blocks)
    def _(step):
        j = step // lane_blocks
        lanes = pl.ds(pl.multiple_of((step % lane_blocks) * 128, 128), 128)
        totals = [None] * D1
        for a in range(R):
            m = mid_s[pl.ds(pl.multiple_of(a * SIDE + j * R, R), R), lanes]
            for i in range(D1):
                term = first_s[i * R + a:i * R + a + 1, lanes] * m
                totals[i] = term if totals[i] is None else totals[i] + term
        for i in range(D1):
            left_s[pl.ds(pl.multiple_of(i * SIDE + j * R, R), R), lanes] = totals[i]

    @pl.loop(0, PAIRS)
    def _(p):
        totals = [None, None]
        for c in range(R):
            term = left_s[pl.ds(p * R + c, 1), :] * last_s[c * D3:(c + 1) * D3, :]
            k = c % 2
            totals[k] = term if totals[k] is None else totals[k] + term
        emb_s[pl.ds(pl.multiple_of(p * D3, D3), D3), :] = totals[0] + totals[1]

    bags = hot(bag[...], samples, F32)
    pooled = dot(bags, emb_s[...], across, HIGH).astype(BF16)
    pre = (
        dot(dense[...], w[:WIDTH, :], plain) + dot(pooled, w[WIDTH:, :], plain)
        + bias[...]
    )
    sig = jax.nn.sigmoid(pre)
    hidden = pre * sig
    logit = jnp.sum(hidden * wout[...], axis=1, keepdims=True)
    rows = lax.broadcasted_iota(jnp.int32, (samples, samples), 0)
    cols = lax.broadcasted_iota(jnp.int32, (samples, samples), 1)
    label = jnp.sum(
        jnp.where(rows == cols, labels[...].astype(F32), 0.0), axis=1, keepdims=True
    )
    dlogit = (jax.nn.sigmoid(logit) - label) / samples
    dpre = dlogit * wout[...] * (sig * (1.0 + pre * (1.0 - sig)))
    low = dpre.astype(BF16)
    places, _ = places_of(c1.shape, c3.shape, w.shape)
    sums_ref[...] = jnp.zeros_like(sums_ref)

    def put(name, row, value):
        for h in range(value.shape[1] // 128):
            at = places[name][h] + row
            sums_ref[at:at + value.shape[0], :] = value[:, h * 128:(h + 1) * 128]

    put("weight", 0, dot(dense[...], low, down))
    put("weight", WIDTH, dot(pooled, low, down))
    put("vectors", 0, jnp.sum(dpre, axis=0, keepdims=True))
    put("vectors", 1, jnp.sum(hidden * dlogit, axis=0, keepdims=True))
    gp = dot(low, w[WIDTH:, :], across)
    block_ref[:samples, :] = gp
    block_ref[samples:, :] = jnp.zeros((block_ref.shape[0] - samples, 128), F32)
    for k, digit in enumerate((bag, d1, d2, d3)):
        for h in range(looks // 128):
            at = samples + k * (looks // 128) + h
            block_ref[at:at + 1, :] = digit[:, h * 128:(h + 1) * 128].astype(F32)
    g_s[...] = dot(gp, bags, down, HIGH)

    grad_left_into(gleft_s, g_s, lastd_s)

    @pl.loop(0, R)
    def _(c):
        totals = [None, None]
        for p in range(PAIRS):
            term = left_s[pl.ds(p * R + c, 1), :] * g_s[p * D3:(p + 1) * D3, :]
            k = p % 2
            totals[k] = term if totals[k] is None else totals[k] + term
        gl_s[pl.ds(pl.multiple_of(c * D3, D3), D3), :] = totals[0] + totals[1]

    @pl.loop(0, R)
    def _(a):
        totals = [None] * D1
        for t in range(0, SIDE, 8):
            m = mid_s[pl.ds(pl.multiple_of(a * SIDE + t, 8), 8), :]
            for i in range(D1):
                term = gleft_s[i * SIDE + t:i * SIDE + t + 8, :] * m
                totals[i] = term if totals[i] is None else totals[i] + term
        for i in range(D1):
            gf_s[pl.ds(i * R + a, 1), :] = jnp.sum(totals[i], axis=0, keepdims=True)

    put("first", 0, dot(hot1.astype(F32), gf_s[...], across, HIGH))
    put("last", 0, dot(hot3.astype(F32), gl_s[...], across, HIGH))


def fetch_then(count, kernel, *refs):
    inputs, rest = refs[:count], refs[count:-count - 1]
    held, sems = refs[-count - 1:-1], refs[-1]
    copies = [
        pltpu.make_async_copy(inputs[k], held[k], sems.at[k]) for k in range(count)]
    for copy in copies:
        copy.start()
    for copy in copies:
        copy.wait()
    kernel(*held, *rest)


def local_part(devices, c1, c2, c3, dense, w, bias, wout, labels, bag, d1, d2, d3):
    samples, looks = dense.shape[0], d1.shape[1]
    shape = lambda *dims: jax.ShapeDtypeStruct(dims, F32)
    scratch = [R * SIDE, D1 * R, R * D3, R * D3, D1 * SIDE, D1 * SIDE, WIDTH, WIDTH, D1 * R, R * D3]
    inputs = (c1, c2, c3, dense, w, bias, wout, labels, bag, d1, d2, d3)
    return pl.pallas_call(
        functools.partial(fetch_then, len(inputs), local_kernel),
        in_specs=[pl.BlockSpec(memory_space=pltpu.HBM)] * len(inputs),
        out_shape=(
            shape(samples + up(4 * looks // 128, 8), WIDTH),
            shape(up(places_of(c1.shape, c3.shape, w.shape)[1], 8 * devices), 128),
        ),
        scratch_shapes=[pltpu.VMEM((rows, looks), F32) for rows in scratch]
        + [pltpu.VMEM(x.shape, x.dtype) for x in inputs]
        + [pltpu.SemaphoreType.DMA((len(inputs),))],
        compiler_params=pltpu.CompilerParams(vmem_limit_bytes=60 * 1024 * 1024),
        name="local",
    )(*inputs)


def middle_kernel(
    window, chunk, samples, looks, r0_ref, c1, c3, blocks, out_ref,
    rank_s, vals_s, g_s, lastd_s, gleft_s,
):
    groups = blocks.shape[0]
    gp = blocks[:, :samples, :].reshape(groups * samples, WIDTH)
    per = looks // 128
    digits = [
        jnp.concatenate(
            [blocks[:, samples + k * per + h, :] for h in range(per)], axis=1
        ).astype(jnp.int32)
        for k in range(4)
    ]
    r0 = r0_ref[0]
    rel = digits[2] - r0
    inside = (rel >= 0) & (rel < window)
    mask = jnp.where(inside, 1.0, 0.0)
    low = mask.astype(BF16)
    tri = jnp.where(
        lax.broadcasted_iota(jnp.int32, (looks, looks), 0)
        < lax.broadcasted_iota(jnp.int32, (looks, looks), 1), 1.0, 0.0).astype(BF16)
    above = jnp.where(
        lax.broadcasted_iota(jnp.int32, (groups, groups), 0)
        > lax.broadcasted_iota(jnp.int32, (groups, groups), 1), 1.0, 0.0).astype(BF16)
    plain, across, down = ((1,), (0,)), ((1,), (1,)), ((0,), (0,))
    before = jnp.sum(dot(above, low, plain), axis=1, keepdims=True)
    rank_s[...] = jnp.where(inside, dot(low, tri, plain) + before, -1.0).astype(jnp.int32)
    count = jnp.sum(jnp.where(inside, 1, 0))
    group = lax.broadcasted_iota(jnp.int32, (groups, looks), 0)
    columns = (digits[0], digits[1], digits[3], group, jnp.where(inside, rel + 1, 0))
    for k, column in enumerate(columns):
        vals_s[:, k:k + 1, :] = column.astype(F32).reshape(groups, 1, looks)
    vals_s[:, len(columns):, :] = jnp.zeros((groups, 8 - len(columns), looks), F32)
    out_ref[...] = jnp.zeros_like(out_ref)
    gp_high = gp.astype(BF16)
    gp_low = (gp - gp_high.astype(F32)).astype(BF16)
    slots = lax.broadcasted_iota(jnp.int32, (chunk, looks), 0)

    def body(step, carry):
        def pick(e, found):
            ranks = rank_s[pl.ds(e, 1), :] - step * chunk
            chosen = jnp.where(slots == ranks, 1.0, 0.0).astype(BF16)
            return found + dot(vals_s[e].astype(BF16), chosen, across)

        found = lax.fori_loop(0, groups, pick, jnp.zeros((8, chunk), F32), unroll=4)
        found = found.astype(jnp.int32)
        bag, d1, d3, owner, rel1 = (found[k:k + 1, :] for k in range(5))
        first = dot(c1[...], hot(d1, c1.shape[0], BF16), down)
        last = dot(c3[...], hot(d3, c3.shape[0], BF16), down)
        lastd_s[...] = by_d3(last.astype(BF16))
        sample = hot(owner * samples + bag, gp.shape[0], BF16)
        g_s[...] = dot(gp_high, sample, down) + dot(gp_low, sample, down)
        grad_left_into(gleft_s, g_s, lastd_s)
        total = out_ref[...]
        for i in range(D1):
            part = first[i * R:(i + 1) * R, :]
            spread = jnp.concatenate(
                [jnp.where(rel1 == r + 1, part, 0.0) for r in range(window)], axis=0
            ).astype(BF16)
            wide = gleft_s[i * SIDE:(i + 1) * SIDE, :]
            high = wide.astype(BF16)
            rest = (wide - high.astype(F32)).astype(BF16)
            total = total + dot(spread, high, across) + dot(spread, rest, across)
        out_ref[...] = total
        return carry

    lax.fori_loop(0, (count + chunk - 1) // chunk, body, 0)


def middle_part(window, samples, looks, r0, c1, c3, blocks):
    groups = blocks.shape[0]
    chunk = 512
    vmem = pl.BlockSpec(memory_space=pltpu.VMEM)
    return pl.pallas_call(
        functools.partial(middle_kernel, window, chunk, samples, looks),
        out_shape=jax.ShapeDtypeStruct((window * R, SIDE), F32),
        in_specs=[pl.BlockSpec(memory_space=pltpu.SMEM), vmem, vmem, vmem],
        out_specs=vmem,
        scratch_shapes=[
            pltpu.VMEM((groups, looks), jnp.int32),
            pltpu.VMEM((groups, 8, looks), F32),
            pltpu.VMEM((WIDTH, chunk), F32),
            pltpu.VMEM((R * D3, chunk), F32),
            pltpu.VMEM((D1 * SIDE, chunk), F32),
        ],
        compiler_params=pltpu.CompilerParams(vmem_limit_bytes=40 << 20),
        name="middle",
    )(r0, c1, c3, blocks)


def levels(nx, ny):
    cores = 2 if nx % 2 == 0 else 1
    return cores, nx // cores, ny


def exchange_kernel(
    nx, ny, block, sums, blocks_ref, total_ref,
    part0, part1, part2, acc0, acc1, *sems,
):
    cores, chips, planes = levels(nx, ny)
    gx, plane = lax.axis_index("gx"), lax.axis_index("gy")
    core, chip = gx % cores, gx // cores

    def on_core(k):
        return (chip * cores + (core + k) % cores, plane)

    def on_chip(k):
        return (((chip + k) % chips) * cores + core, plane)

    def on_plane(k):
        return (gx, (plane + k) % planes)

    def remote(src, dst, number, k, peer):
        return pltpu.make_async_remote_copy(
            src_ref=src, dst_ref=dst,
            send_sem=sems[2 * number].at[k], recv_sem=sems[2 * number + 1].at[k],
            device_id=peer, device_id_type=pl.DeviceIdType.MESH)

    def stage(number, size, copy):
        for k in range(1, size):
            copy(k, k).start()

        def arrived():
            for k in range(1, size):
                copy(k, -k).wait_recv()

        def sent():
            for k in range(1, size):
                copy(k, k).wait_send()

        return arrived, sent

    def spread(ref, number, size, mine, view, peer):
        def copy(k, off):
            at = mine if off > 0 else (mine + off + size) % size
            return remote(view(ref, at), view(ref, at), number, k, peer(k))
        return stage(number, size, copy)

    barrier = pltpu.get_barrier_semaphore()
    greeted = 0
    for size, peer in ((cores, on_core), (chips, on_chip), (planes, on_plane)):
        for k in range(1, size):
            pl.semaphore_signal(
                barrier, inc=1, device_id=peer(k), device_id_type=pl.DeviceIdType.MESH)
            greeted += 1
    pl.semaphore_wait(barrier, greeted)

    sent = []

    def go(pair):
        sent.append(pair[1])
        return pair[0]

    def block_copy(k, off):
        at = plane if off > 0 else (plane + off + planes) % planes
        return remote(block, blocks_ref.at[core, chip, at], 3, k, on_plane(k))

    arrived_r0 = go(stage(0, cores, lambda k, off: remote(
        sums.at[(core + k) % cores], part0.at[k], 0, k, on_core(k))))
    arrived_bz = go(stage(3, planes, block_copy))
    blocks_ref[core, chip, plane] = block[...]

    arrived_r0()
    total = sums[core]
    for k in range(1, cores):
        total = total + part0[k]
    acc0[...] = total
    arrived_r1 = go(stage(1, chips, lambda k, off: remote(
        acc0.at[(chip + k) % chips], part1.at[k], 1, k, on_chip(k))))
    arrived_bz()
    arrived_b1 = go(spread(
        blocks_ref, 4, chips, chip, lambda r, at: r.at[core, at], on_chip))

    arrived_r1()
    total = acc0[chip]
    for k in range(1, chips):
        total = total + part1[k]
    acc1[...] = total
    arrived_r2 = go(stage(2, planes, lambda k, off: remote(
        acc1.at[(plane + k) % planes], part2.at[k], 2, k, on_plane(k))))
    arrived_r2()
    total = acc1[plane]
    for k in range(1, planes):
        total = total + part2[k]
    total_ref[core, chip, plane] = total
    go(spread(
        total_ref, 5, planes, plane, lambda r, at: r.at[core, chip, at], on_plane))()
    arrived_a1 = go(spread(
        total_ref, 6, chips, chip, lambda r, at: r.at[core, at], on_chip))
    arrived_b1()
    arrived_b0 = go(spread(blocks_ref, 7, cores, core, lambda r, at: r.at[at], on_core))
    arrived_a1()
    arrived_a0 = go(spread(total_ref, 8, cores, core, lambda r, at: r.at[at], on_core))
    arrived_b0()
    arrived_a0()
    for wait in sent:
        wait()


def exchange(nx, ny, block, sums):
    cores, chips, planes = levels(nx, ny)
    part = sums.shape[0] // (nx * ny)
    vmem = pl.BlockSpec(memory_space=pltpu.VMEM)
    shape = (cores, chips, planes, part, 128)
    scratch = [
        (cores, *shape[1:]), (chips, *shape[2:]), (planes, *shape[3:]), shape[1:], shape[2:]]
    sizes = (cores, chips, planes, planes, chips, planes, chips, cores, cores)
    blocks, total = pl.pallas_call(
        functools.partial(exchange_kernel, nx, ny),
        out_shape=(
            jax.ShapeDtypeStruct((cores, chips, planes, *block.shape), F32),
            jax.ShapeDtypeStruct(shape, F32),
        ),
        in_specs=[vmem, vmem],
        out_specs=(vmem, vmem),
        scratch_shapes=[pltpu.VMEM(dims, F32) for dims in scratch]
        + [pltpu.SemaphoreType.DMA((size,)) for size in sizes for _ in range(2)],
        compiler_params=pltpu.CompilerParams(
            collective_id=0, has_side_effects=True, vmem_limit_bytes=24 << 20),
        name="exchange",
    )(block, sums.reshape(shape))
    return blocks.reshape(-1, *block.shape), total


def cut(start, share, core_shapes, window, r0, first_sum, middle_rows, last_sum):
    n1 = core_shapes[0][0] * core_shapes[0][1]
    row = core_shapes[1][1]
    n2 = core_shapes[1][0] * row
    own_first = lax.dynamic_slice(
        jnp.pad(first_sum, (0, share)), (jnp.minimum(start, n1),), (share,))
    own_middle = lax.dynamic_slice(
        jnp.pad(middle_rows, (share, share)),
        (jnp.clip(start - n1 - r0 * row + share, 0, share + window * row),), (share,))
    own_last = lax.dynamic_slice(
        jnp.pad(last_sum, (share, 0)),
        (jnp.clip(start - n1 - n2 + share, 0, last_sum.shape[0]),), (share,))
    return own_first + own_middle + own_last


def per_device(nx, ny, c1, c2, c3, dense, w, bias, wout, labels, bag, d1, d2, d3):
    devices = nx * ny
    total = c1.size + c2.size + c3.size
    share = total // devices
    row = c2.shape[1]
    window = min(-(-share // row) + 1, c2.shape[0])
    start = (lax.axis_index("gx") * ny + lax.axis_index("gy")) * share
    r0 = jnp.clip((start - c1.size) // row, 0, c2.shape[0] - window)
    block, sums = local_part(
        devices, c1, c2, c3, dense, w, bias[None], wout[None], labels[None], bag, d1, d2, d3)
    blocks, sums = exchange(nx, ny, block, sums)
    rows = middle_part(window, dense.shape[0], d1.shape[1], r0[None], c1, c3, blocks)
    sums = sums.reshape(-1, 128)
    places, _ = places_of(c1.shape, c3.shape, w.shape)

    def take(name, count):
        return jnp.concatenate([sums[at:at + count] for at in places[name]], axis=1)

    core = cut(start, share, (c1.shape, c2.shape, c3.shape), window, r0,
               take("first", c1.shape[0]).reshape(-1), rows.reshape(-1),
               take("last", c3.shape[0]).reshape(-1))
    return core, jnp.concatenate([take("weight", w.shape[0]), take("vectors", 2)], axis=0)


def one_hot(digits, count, kind):
    return (digits[:, None] == jnp.arange(count, dtype=jnp.int32)[None, :]).astype(kind)


def slices(digits, core):
    return jnp.dot(
        one_hot(digits, core.shape[0], jnp.bfloat16), core, preferred_element_type=jnp.float32
    )


def factors(digits, cores):
    high = lax.Precision.HIGHEST
    first = slices(digits[0], cores[0]).reshape(-1, D1, R)
    middle = slices(digits[1], cores[1]).reshape(-1, R, D2 * R)
    last = slices(digits[2], cores[2]).reshape(-1, R, D3)
    left = jnp.einsum("nia,nab->nib", first, middle, precision=high).reshape(-1, D1 * D2, R)
    return (first, middle, last, left)


def top_total(top_local):
    return lax.psum(top_local, ("gx", "gy"))


def per_device_dense(
    core_one,
    core_two,
    core_three,
    dense_rows,
    w_top,
    bias_top,
    w_out,
    labels,
    bag_ids,
    digit_one,
    digit_two,
    digit_three,
):
    high = lax.Precision.HIGHEST
    cores = (core_one, core_two, core_three)
    digits = jnp.stack([digit_one[0], digit_two[0], digit_three[0]])
    looks = digits.shape[1]
    block = min(256, looks)
    blocks = looks // block
    blocked = digits.reshape(3, blocks, block).transpose(1, 0, 2)
    width = D1 * D2 * D3

    def forward(carry, part):
        first, middle, last, left = factors(part, cores)
        return (carry, jnp.einsum("npa,nad->npd", left, last, precision=high).reshape(block, width))

    _, embedded = lax.scan(forward, jnp.zeros((), jnp.float32), blocked)
    embedded = embedded.reshape(looks, width)
    samples = dense_rows.shape[0]
    bag_table = one_hot(bag_ids[0], samples, jnp.float32)
    pooled = jnp.dot(bag_table.T, embedded, precision=high)
    joined = jnp.concatenate([dense_rows, pooled.astype(jnp.bfloat16)], axis=1)
    pre = jnp.dot(joined, w_top, preferred_element_type=jnp.float32) + bias_top[None, :]
    sig = jax.nn.sigmoid(pre)
    hidden = pre * sig
    logit = jnp.dot(hidden, w_out, precision=high)
    dlogit = (jax.nn.sigmoid(logit) - labels.astype(jnp.float32)) / samples
    dpre = dlogit[:, None] * w_out[None, :] * (sig * (1.0 + pre * (1.0 - sig)))
    dpre_low = dpre.astype(jnp.bfloat16)
    grad_weight = jnp.dot(joined.T, dpre_low, preferred_element_type=jnp.float32)
    grad_bias = jnp.sum(dpre, axis=0)
    grad_output = jnp.sum(hidden * dlogit[:, None], axis=0)
    top_local = jnp.concatenate([grad_weight, grad_bias[None, :], grad_output[None, :]], axis=0)
    grad_pooled = jnp.dot(dpre_low, w_top[width:].T, preferred_element_type=jnp.float32)
    grad_embedded = jnp.dot(bag_table, grad_pooled, precision=high).reshape(blocks, block, width)

    def backward(totals, inputs):
        part, grad_block = inputs
        first, middle, last, left = factors(part, cores)
        grad_view = grad_block.reshape(block, D1 * D2, D3)
        grad_last = jnp.einsum("npa,npd->nad", left, grad_view, precision=high)
        grad_left = jnp.einsum("npd,nad->npa", grad_view, last, precision=high).reshape(
            block, D1, D2 * R
        )
        grad_first = jnp.einsum("nib,nab->nia", grad_left, middle, precision=high)
        grad_middle = jnp.einsum("nia,nib->nab", first, grad_left, precision=high)
        pieces = (
            grad_first.reshape(block, -1),
            grad_middle.reshape(block, -1),
            grad_last.reshape(block, -1),
        )
        updated = tuple(
            (
                total
                + jnp.dot(
                    one_hot(part[number], cores[number].shape[0], jnp.float32).T,
                    pieces[number],
                    precision=high,
                )
                for number, total in enumerate(totals)
            )
        )
        return (updated, None)

    start = tuple((jnp.zeros(core.shape, jnp.float32) for core in cores))
    totals, _ = lax.scan(backward, start, (blocked, grad_embedded))
    flat = jnp.concatenate([total.reshape(-1) for total in totals])
    core_grad = lax.psum_scatter(flat, ("gx", "gy"), scatter_dimension=0, tiled=True)
    top_grad = top_total(top_local)
    return (core_grad, top_grad)


def solution(mesh):
    nx, ny = mesh.shape["gx"], mesh.shape["gy"]
    whole, split, rows = P(), P(AXES), P(AXES, None)

    def step(*args):
        cores, dense = args[:3], args[3]
        if dense.size < sum(core.size for core in cores):
            body = functools.partial(per_device, nx, ny)
        else:
            body = per_device_dense
        return jax.shard_map(
            body,
            mesh=mesh,
            in_specs=(
                whole, whole, whole, rows, whole, whole, whole, split,
                rows, rows, rows, rows,
            ),
            out_specs=(split, whole),
            check_vma=False,
        )(*args)

    return step
```
